32 devices in a mesh: gx: 2 (over core), gy: 2 (over x), gz: 8 (over z, y).
Axes of the slice: x: 2, y: 2, z: 4, core: 2. Of those that a mesh axis runs over, the one named last changes fastest.
Arguments:
- old_pos: float32 [3, 32768], P(None, ('gx', 'gy', 'gz')), may hold values from -6 to 6
- new_pos: float32 [3, 32768], P(None, ('gx', 'gy', 'gz')), may hold values from -6 to 6
- inv_mass: float32 [32768], P(('gx', 'gy', 'gz')), may hold values from 0.05 to 1
- rest_length: float32 [32768], P(('gx', 'gy', 'gz')), may hold values from 0.8 to 1.6
- bond_pairs: int32 [2, 32768], P(None, ('gx', 'gy', 'gz')), may hold values from 0 to 1311, as said below
- live: int32 [32768], P(('gx', 'gy', 'gz')), may hold values from 0 to 1, as said below
- send_index: int32 [192, 48], P(('gx', 'gy', 'gz')), may hold values from 0 to 1023, as said below
Outputs:
- displacement: float32 [3, 32768], P(None, ('gx', 'gy', 'gz'))
- multipliers: float32 [32768], P(('gx', 'gy', 'gz'))
The draws below stay inside these ranges and needn't reach their ends.
Inputs may be any that keep to these rules, and one draw needn't show every extreme that they name: `bond_pairs`: in domain k's slots, row 0 is an own atom (0 to 1023). Row 1 indexes the domain's extended list: its own atoms, then six blocks of 48 received atoms, block 2a + s holding, in order, list 2a + s of the neighbour one step down (s = 0) or up (s = 1) along axis a. Every atom is in at most two live constraints, each received atom is the second atom of at most one live constraint, and exactly 216 live constraints of each domain name a received atom. `live`: padding slots change nothing. `send_index`: rows 6k to 6k + 5 are domain k's lists of own atoms; list 2a + s goes to the neighbour one step up (s = 0) or down (s = 1) along axis a, periodically. The 288 entries of a domain are distinct.
All inputs are finite; a program needn't handle non-finite values.
Results may differ from the reference program's by a relative error of at most 0.0001.
Values sent between devices are 32-bit elements; how exact they have to be, the bound alone decides.
No kernel may reach another device: no remote copies, remote signals or barrier semaphores. Data moves between devices by JAX's collectives and lax.ppermute only.
A program may use at most 64 MiB of HBM per device.

```python
import math
import jax
import jax.numpy as jnp
from jax import lax

ATOMS_DEV = 1024
HALO_ROWS = 48
CHAIN_HEADS = 384
CROSS_BONDS = 216
ORDER = 4
DOMAINS = 32
ATOMS = 32768
N_GX = 2
N_GY = 2
N_GZ = 8


def one_domain(key):
    keys = jax.random.split(key, 6)
    position = jnp.arange(ATOMS_DEV, dtype=jnp.int32)
    atom_slot = jax.random.permutation(keys[0], ATOMS_DEV).astype(jnp.int32)
    ranking = jax.random.permutation(keys[1], ATOMS_DEV).astype(jnp.int32)
    heading = (ranking < CHAIN_HEADS) | (position == 0)
    ending = jnp.concatenate([heading[1:], jnp.ones((1,), dtype=bool)])
    tiebreak = jax.random.permutation(keys[2], ATOMS_DEV).astype(jnp.int32)
    end_score = ending.astype(jnp.int32) * (1 << 24) + tiebreak
    unused_end, cross_pos = lax.top_k(end_score, CROSS_BONDS)
    halo_slot = jax.random.permutation(keys[3], 6 * HALO_ROWS).astype(jnp.int32)[:CROSS_BONDS] + ATOMS_DEV
    following = jnp.roll(atom_slot, -1)
    second_atom = jnp.where(ending, 0, following).astype(jnp.int32)
    second_atom = second_atom.at[cross_pos].set(halo_slot)
    alive = jnp.where(ending, 0, 1).astype(jnp.int32).at[cross_pos].set(1)
    ordering = jax.random.permutation(keys[4], ATOMS_DEV).astype(jnp.int32)
    first_atom = atom_slot[ordering]
    second_atom = second_atom[ordering]
    alive = alive[ordering]
    head_tie = jax.random.permutation(keys[5], ATOMS_DEV).astype(jnp.int32)
    head_score = heading.astype(jnp.int32) * (1 << 24) + head_tie
    unused_head, head_pos = lax.top_k(head_score, 6 * HALO_ROWS)
    sending = atom_slot[head_pos].reshape(6, HALO_ROWS)
    return (first_atom, second_atom, alive, sending)


def all_domains(key):
    numbers = jnp.arange(DOMAINS, dtype=jnp.int32)
    domain_keys = jax.vmap(lambda number: jax.random.fold_in(key, number))(numbers)
    return jax.vmap(one_domain)(domain_keys)


def draw_bond_pairs(key, part):
    first_atom, second_atom, alive, sending = all_domains(key)
    return jnp.stack([first_atom.reshape(-1), second_atom.reshape(-1)], 0).astype(jnp.int32)


def draw_live(key, part):
    first_atom, second_atom, alive, sending = all_domains(key)
    return alive.reshape(-1).astype(jnp.int32)


def draw_send_index(key, part):
    first_atom, second_atom, alive, sending = all_domains(key)
    return sending.reshape(DOMAINS * 6, HALO_ROWS).astype(jnp.int32)


def block_levels(stream_key, dims, cuts, low, high):
    def one(dim, parts):
        draws = jax.random.uniform(jax.random.fold_in(jax.random.fold_in(stream_key, 6), dim), (parts,), jnp.float32, low / len(cuts), high / len(cuts))
        return jnp.repeat(jnp.exp(draws), dims[dim] // parts).reshape((-1,) + (1,) * (len(dims) - dim - 1))

    level = one(*cuts[0])
    for cut in cuts[1:]:
        level = level * one(*cut)
    return level


def normal_values(key, dims, scale, most, cuts=(), kind=jnp.bfloat16):
    drawn = scale * jax.random.normal(key, dims, jnp.float32)
    if cuts:
        drawn = drawn * block_levels(key, dims, cuts, -0.22, 0.18)
    return jnp.clip(drawn, -most, most).astype(kind)


def setup_inputs(seed: int = 0) -> dict:
    streams_of = jax.random.split(jax.random.key(seed), 8)
    return {
        "old_pos": normal_values(streams_of[0], (3, ATOMS), 1.0, 6.0, ((1, 32),), jnp.float32),
        "new_pos": normal_values(streams_of[1], (3, ATOMS), 1.0, 6.0, ((1, 32),), jnp.float32),
        "inv_mass": jnp.clip(jnp.exp(math.log(1.0) - 2.9957323 * jax.random.uniform(streams_of[2], (ATOMS,), jnp.float32) ** block_levels(streams_of[2], (ATOMS,), ((0, 32),), -0.2, 0.2)), 0.05, 1.0),
        "rest_length": jnp.clip(0.8 + 0.8 * jax.random.uniform(streams_of[3], (ATOMS,), jnp.float32) ** block_levels(streams_of[3], (ATOMS,), ((0, 32),), -0.2, 0.2), 0.8, 1.6),
        "bond_pairs": draw_bond_pairs(jax.random.fold_in(streams_of[7], 71), 0),
        "live": draw_live(jax.random.fold_in(streams_of[7], 71), 0),
        "send_index": draw_send_index(jax.random.fold_in(streams_of[7], 71), 0),
    }


def owners(bond_pairs, send_index):
    slot_index = jnp.arange(ATOMS, dtype=jnp.int32)
    domain = slot_index // ATOMS_DEV
    first_atom = domain * ATOMS_DEV + bond_pairs[0].astype(jnp.int32)
    local_second = bond_pairs[1].astype(jnp.int32)
    remote = local_second >= ATOMS_DEV
    offset = jnp.maximum(local_second - ATOMS_DEV, 0)
    block = offset // HALO_ROWS
    row_index = offset % HALO_ROWS
    coord_x = domain // (N_GY * N_GZ)
    coord_y = domain // N_GZ % N_GY
    coord_z = domain % N_GZ
    stride = jnp.where(block % 2 == 0, -1, 1)
    axis_pick = block // 2
    source_x = (coord_x + jnp.where(axis_pick == 0, stride, 0)) % N_GX
    source_y = (coord_y + jnp.where(axis_pick == 1, stride, 0)) % N_GY
    source_z = (coord_z + jnp.where(axis_pick == 2, stride, 0)) % N_GZ
    source = (source_x * N_GY + source_y) * N_GZ + source_z
    sent_atom = send_index[source * 6 + block, row_index].astype(jnp.int32)
    second_atom = jnp.where(remote, source * ATOMS_DEV + sent_atom, domain * ATOMS_DEV + local_second)
    return (first_atom, second_atom)

def reference(old_pos, new_pos, inv_mass, rest_length, bond_pairs, live, send_index):
    first_atom, second_atom = owners(bond_pairs, send_index)

    def across_bond(field):
        return field[:, first_atom] - field[:, second_atom]
    old_span = across_bond(old_pos)
    unit_dir = old_span / jnp.sqrt(lax.optimization_barrier(jnp.sum(old_span * old_span, 0)) + 0.25)
    scaling = live.astype(jnp.float32) / jnp.sqrt(inv_mass[first_atom] + inv_mass[second_atom])

    def atom_shift(values):
        contrib = unit_dir * (scaling * values)[None]
        blank = jnp.zeros((3, ATOMS), jnp.float32)
        summed = blank.at[:, first_atom].add(contrib).at[:, second_atom].add(-contrib)
        return inv_mass[None] * summed

    def coupling(values):
        return values - scaling * lax.optimization_barrier(jnp.sum(unit_dir * across_bond(atom_shift(values)), 0))

    def expansion(start):
        series = start
        current = start
        for repeat in range(ORDER):
            current = coupling(current)
            series = series + current
        return series
    right_side = scaling * (lax.optimization_barrier(jnp.sum(unit_dir * across_bond(new_pos), 0)) - rest_length)
    first_sol = expansion(right_side)
    shifted_pos = new_pos - atom_shift(first_sol)
    stretch = across_bond(shifted_pos)
    length_sq = lax.optimization_barrier(jnp.sum(stretch * stretch, 0))
    floor_sq = 0.25 * rest_length * rest_length
    target = jnp.sqrt(jnp.maximum(2.0 * rest_length * rest_length - length_sq, floor_sq))
    second_sol = expansion(scaling * (rest_length - target))
    final_pos = shifted_pos - atom_shift(second_sol)
    return (final_pos - new_pos, first_sol + second_sol)
```

```python
import functools
import itertools

import jax
import jax.numpy as jnp
import numpy as np
from jax import lax
from jax.experimental import pallas as pl
from jax.experimental.pallas import tpu as pltpu
from jax.sharding import PartitionSpec as P

ORDER = 4
AXES = ("gx", "gy", "gz")
LANES = 128
HALF = LANES // 2
SUB = 8
CHUNK = 8
FIELDS = 12
REACH = 2 * (ORDER + 1)
VMEM = pl.BlockSpec(memory_space=pltpu.VMEM)
SMEM = pl.BlockSpec(memory_space=pltpu.SMEM)


def wide(row):
    return jnp.broadcast_to(row, (SUB, LANES))


def pick(tables, row, lane):
    total = jnp.zeros((SUB, LANES), jnp.float32)
    for number, load in tables.items():
        got = jnp.take_along_axis(wide(load()), lane, axis=1, mode="promise_in_bounds")
        total = jnp.where(row == number, got.astype(jnp.float32), total)
    return total


def flat_rows(ref, q):
    return {r: functools.partial(lambda q, r: ref[q : q + 1, r * LANES : (r + 1) * LANES], q, r) for r in range(SUB)}


def tile_rows(ref, base=0):
    return {r: functools.partial(lambda r: ref[base + r : base + r + 1, :], r) for r in range(SUB)}


def stack_rows(ref, q, hold):
    for r in range(SUB):
        hold[r : r + 1, :] = ref[q : q + 1, r * LANES : (r + 1) * LANES]
    return hold[...]


def sent_kernel(old, new, mass, send, out_x, out_y, out_z, where, pad):
    width = send.shape[1]
    pad[...] = jnp.zeros_like(pad)
    pad[0:6, 0:width] = send[...]
    low = pad[...]
    high = pltpu.roll(low, HALF, 1)
    where[...] = jnp.zeros_like(where)
    for a in range(3):
        where[a : a + 1, :] = low[2 * a : 2 * a + 1] + high[2 * a + 1 : 2 * a + 2]
    index = where[...]
    row, lane = index >> 7, index & (LANES - 1)
    tables = [flat_rows(old, q) for q in range(3)] + [flat_rows(new, q) for q in range(3)] + [tile_rows(mass)]
    outs = (out_x, out_y, out_z)
    for a in range(3):
        outs[a][...] = jnp.zeros_like(outs[a])
    for f, table in enumerate(tables):
        got = pick(table, row, lane)
        for a in range(3):
            outs[a][f : f + 1, :] = got[a : a + 1, :]


def second_place(second, width):
    atoms = SUB * LANES
    slot = second - atoms
    block = jnp.zeros_like(second)
    for b in range(1, 6):
        block = block + (slot >= b * width).astype(jnp.int32)
    lane = slot - block * width + (block & 1) * HALF
    remote = second >= atoms
    row = jnp.where(remote, 12 + (block >> 1), second >> 7)
    return row, jnp.where(remote, lane, second & (LANES - 1))


def nt_dot(a, b):
    return lax.dot_general(a, b, (((1,), (1,)), ((), ())), preferred_element_type=jnp.float32)


def split_codes(hit, code):
    code = jnp.broadcast_to(code, hit.shape)
    zero = jnp.zeros_like(code)
    both = jnp.concatenate([jnp.where(hit, code >> 4, zero), jnp.where(hit, code & 15, zero)], 0)
    return both.astype(jnp.float32).astype(jnp.bfloat16)


def lane_hits(lane, count):
    hits = lax.broadcasted_iota(jnp.int32, (LANES, count), 0) == jnp.broadcast_to(lane, (LANES, count))
    return jnp.where(hits, 1.0, 0.0).astype(jnp.bfloat16)


def link_kernel(width, bonds, live_row, live, where, links, hold_a, hold_b, s_ref):
    atoms = SUB * LANES
    first_row = bonds[0:1, :]
    second_row = bonds[1:2, :]
    usable = (live_row[...] != 0) & (first_row != second_row)
    node = lax.broadcasted_iota(jnp.int32, (1, atoms), 1)
    targets = lax.broadcasted_iota(jnp.int32, (2 * SUB, atoms), 0)
    total = jnp.zeros((4 * SUB, LANES), jnp.float32)
    places = ((first_row >> 7, first_row & (LANES - 1)), second_place(second_row, width))
    for end, (row, lane) in enumerate(places):
        row = jnp.where(usable, row, -1)
        hit = targets == jnp.broadcast_to(row, targets.shape)
        total = total + nt_dot(split_codes(hit, 2 * node + end + 1), lane_hits(lane, atoms))
    sums = 16.0 * total[: 2 * SUB] + total[2 * SUB :]

    index = where[...]
    lanes = lax.broadcasted_iota(jnp.int32, (1, LANES), 1)
    valid = ((lanes & (HALF - 1)) < width)
    small = lax.broadcasted_iota(jnp.int32, (SUB, LANES), 0)
    slots = jnp.zeros((2 * SUB, LANES), jnp.float32)
    for a in range(3):
        one = index[a : a + 1, :]
        row = jnp.where(valid, one >> 7, -1)
        hit = small == jnp.broadcast_to(row, small.shape)
        slots = slots + nt_dot(split_codes(hit, (SUB + a) * LANES + lanes + 1), lane_hits(one & (LANES - 1), LANES))
    sent_slot = 16.0 * slots[:SUB] + slots[SUB:]
    s_ref[0:SUB, :] = 4096.0 * sums[:SUB] + sent_slot
    out_code = sums[SUB:]

    first = stack_rows(bonds, 0, hold_a)
    second = stack_rows(bonds, 1, hold_b)
    alive = (live[...] != 0) & (first != second)
    me = lax.broadcasted_iota(jnp.int32, (SUB, LANES), 0) * LANES + lax.broadcasted_iota(jnp.int32, (SUB, LANES), 1)
    none = 2 * (2 * atoms - 1)
    table = tile_rows(s_ref)
    srow, slane = second_place(second, width)
    for end, (row, lane) in enumerate(((first >> 7, first & (LANES - 1)), (srow, slane))):
        both = pick(table, row, lane).astype(jnp.int32)
        code = (both >> 12) - (2 * me + end + 1)
        ghost = both & 4095
        link = jnp.where(code > 0, code - 1, jnp.where(ghost > 0, 2 * (ghost - 1), none))
        if end == 1:
            link = jnp.where(row >= SUB, 2 * (row * LANES + lane), link)
        links[end * SUB : (end + 1) * SUB, :] = jnp.where(alive, link, none).astype(jnp.float32)
    sent = pick(table, index >> 7, index & (LANES - 1)).astype(jnp.int32) >> 12
    sublane = lax.broadcasted_iota(jnp.int32, (SUB, LANES), 0)
    in_row = (sublane < 3) & ((lax.broadcasted_iota(jnp.int32, (SUB, LANES), 1) & (HALF - 1)) < width)
    ends = jnp.where(in_row, sent - 1, jnp.where(sublane >= 4, out_code.astype(jnp.int32) - 1, -1))
    links[2 * SUB : 3 * SUB, :] = ends.astype(jnp.float32)


def node_kernel(width, old, new, mass, rest, live, bonds, links, *refs):
    arrived = refs[:6]
    pub, hold_a, hold_b, got_ref = refs[6:]
    first = stack_rows(bonds, 0, hold_a)
    second = stack_rows(bonds, 1, hold_b)
    lower = lax.broadcasted_iota(jnp.int32, (1, LANES), 1) < HALF
    for a in range(3):
        got_ref[a * SUB : (a + 1) * SUB, :] = jnp.where(lower, arrived[2 * a][...], arrived[2 * a + 1][...])
    row, lane = first >> 7, first & (LANES - 1)
    srow, slane = second_place(second, width)
    tables = [flat_rows(old, q) for q in range(3)] + [flat_rows(new, q) for q in range(3)] + [tile_rows(mass)]
    firsts, seconds = [], []
    for f, table in enumerate(tables):
        firsts.append(pick(table, row, lane))
        more = dict(table)
        for a in range(3):
            more[12 + a] = functools.partial(lambda at: got_ref[at : at + 1, :], a * SUB + f)
        seconds.append(pick(more, srow, slane))
    span = [x - y for x, y in zip(firsts, seconds)]
    alive = live[...].astype(jnp.float32)
    scaling = alive * lax.rsqrt(firsts[6] + seconds[6])
    norm = lax.rsqrt(span[0] * span[0] + span[1] * span[1] + span[2] * span[2] + 0.25)
    values = [scaling * norm * span[q] for q in range(3)]
    values = values + [scaling * span[3 + q] for q in range(3)]
    values = values + [scaling * rest[...], firsts[6], seconds[6]]
    for f, value in enumerate(values):
        pub[f * SUB : (f + 1) * SUB, :] = value
    pub[9 * SUB : 12 * SUB, :] = links[...]


def place(dart):
    return dart >> 8, (dart >> 1) & (LANES - 1)


def main_kernel(
    counts, split, width, source, slot, near, bonds, mass, where, *refs
):
    shifts = len(split)
    pubs = refs[:shifts]
    (
        out_disp, out_mult, u_ref, n_ref, rho_ref, mf_ref, mg_ref, p_ref, e_ref,
        eu_ref, g_ref, w_ref, diag_ref, xa, xb, one_ref, two_ref, ep_ref, hold_a, hold_b,
    ) = refs[shifts:]

    start = 0
    for shift in range(shifts):
        pub = pubs[shift]

        def load(j, carry, pub=pub):
            s = source[j]
            d = slot[j]
            field = [pub[s, f * SUB : (f + 1) * SUB, :] for f in range(FIELDS)]
            u, n = field[0:3], field[3:6]
            both = field[7] + field[8]
            root = both * lax.rsqrt(both)
            size = u[0] * u[0] + u[1] * u[1] + u[2] * u[2]
            dot = u[0] * n[0] + u[1] * n[1] + u[2] * n[2]
            value = dot * root - field[6]
            diag_ref[d] = 1.0 - both * size
            xa[d] = value
            one_ref[d] = value
            for q in range(3):
                u_ref[d, q] = u[q]
                n_ref[d, q] = n[q]
            rho_ref[d] = field[6]
            mf_ref[d] = field[7]
            mg_ref[d] = field[8]
            p_ref[d, 0] = field[9].astype(jnp.int32)
            p_ref[d, 1] = field[10].astype(jnp.int32)
            dart = field[11].astype(jnp.int32)
            e_ref[d] = dart
            row, lane = place(dart)
            sign = jnp.where((dart & 1) == 1, -1.0, 1.0)
            for q in range(3):
                table = {r: functools.partial(lambda q, r: pub[s, q * SUB + r : q * SUB + r + 1, :], q, r) for r in range(SUB)}
                eu_ref[d, q] = sign * pick(table, row, lane)
            return carry

        lax.fori_loop(start, start + split[shift], load, 0)
        start = start + split[shift]

    lower = lax.broadcasted_iota(jnp.int32, (SUB, LANES), 1) < HALF

    def chunks(count, body):
        steps = -(-count // CHUNK)

        def step(c, carry):
            done = [body(c * CHUNK + k) for k in range(CHUNK)]
            for finish in done:
                finish()
            return carry

        if steps == 1:
            step(0, 0)
        else:
            lax.fori_loop(0, steps, step, 0)

    def table_of(i, own, ghost):
        rows = {r: functools.partial(own, i, r) for r in range(SUB)}
        for a in range(3):
            down, up = near[6 * i + 2 * a], near[6 * i + 2 * a + 1]

            def into(a=a, down=down, up=up):
                return jnp.where(lower, wide(ghost(up, 4 + a)), wide(ghost(down, 4 + a)))

            def away(a=a, down=down, up=up):
                return jnp.where(lower, wide(ghost(down, a)), wide(ghost(up, a)))

            rows[SUB + a] = into
            rows[SUB + 4 + a] = away
        return rows

    def pick_two(i, own, ghost):
        rows = table_of(i, own, ghost)
        places = [place(p_ref[i, 0]), place(p_ref[i, 1])]
        totals = [jnp.zeros((SUB, LANES), jnp.float32)] * 2
        for number, make in rows.items():
            data = wide(make())
            for end in range(2):
                row, lane = places[end]
                got = jnp.take_along_axis(data, lane, axis=1, mode="promise_in_bounds")
                totals[end] = jnp.where(row == number, got, totals[end])
        return totals

    def couple_setup(i):
        u = [u_ref[i, q] for q in range(3)]
        mf, mg = mf_ref[i], mg_ref[i]
        signs = [mf * jnp.where((p_ref[i, 0] & 1) == 1, -1.0, 1.0), -mg * jnp.where((p_ref[i, 1] & 1) == 1, -1.0, 1.0)]
        weights = [jnp.zeros((SUB, LANES), jnp.float32)] * 2
        pulls = []
        for q in range(3):
            got = pick_two(
                i, lambda i, r, q=q: u_ref[i, q, r : r + 1, :], lambda i, r, q=q: eu_ref[i, q, r : r + 1, :]
            )
            for end in range(2):
                pull = signs[end] * got[end]
                weights[end] = weights[end] + u[q] * pull
                pulls.append((end * 3 + q, pull))

        def finish():
            for at, pull in pulls:
                g_ref[i, at] = pull
            for end in range(2):
                w_ref[i, end] = weights[end]

        return finish

    chunks(counts[REACH - 1], couple_setup)

    def send_ends(x, count):
        def body(i):
            row, lane = place(e_ref[i])
            got = pick({r: functools.partial(lambda r: x[i, r : r + 1, :], r) for r in range(SUB)}, row, lane)

            def finish():
                ep_ref[i] = got

            return finish

        chunks(count, body)

    def own_of(x):
        return lambda i, r: x[i, r : r + 1, :]

    def ghost_value(i, r):
        return ep_ref[i, r : r + 1, :]

    def expand(current, following, total, reach):
        for term in range(ORDER):
            send_ends(current, counts[reach - term])

            def body(i, current=current, following=following):
                got = pick_two(i, own_of(current), ghost_value)
                value = diag_ref[i] * current[i] - w_ref[i, 0] * got[0] - w_ref[i, 1] * got[1]

                def finish():
                    following[i] = value
                    total[i] = total[i] + value

                return finish

            chunks(counts[reach - term - 1], body)
            current, following = following, current

    expand(xa, xb, one_ref, REACH)
    send_ends(one_ref, counts[ORDER + 2])

    def correct(i):
        got = pick_two(i, own_of(one_ref), ghost_value)
        both = mf_ref[i] + mg_ref[i]
        scaling = lax.rsqrt(both)
        mine = both * one_ref[i]
        length = jnp.zeros((SUB, LANES), jnp.float32)
        for q in range(3):
            part = n_ref[i, q] - scaling * (u_ref[i, q] * mine + g_ref[i, q] * got[0] + g_ref[i, 3 + q] * got[1])
            length = length + part * part
        rho = rho_ref[i]
        square = rho * rho
        value = rho - jnp.sqrt(jnp.maximum(2.0 * square - length, 0.25 * square))

        def finish():
            xa[i] = value
            two_ref[i] = value

        return finish

    chunks(counts[ORDER + 1], correct)
    expand(xa, xb, two_ref, ORDER + 1)

    def join(i):
        value = one_ref[i] + two_ref[i]

        def finish():
            xa[i] = value

        return finish

    chunks(counts[1], join)
    send_ends(xa, counts[1])

    multiplier = xa[0]
    out_mult[...] = multiplier
    first = stack_rows(bonds, 0, hold_a)
    second = stack_rows(bonds, 1, hold_b)
    small = lax.broadcasted_iota(jnp.int32, (SUB, LANES), 0)
    tall = lax.broadcasted_iota(jnp.int32, (LANES, LANES), 0)
    force = [u_ref[0, q] * multiplier for q in range(3)]
    total = jnp.zeros((3 * SUB, LANES), jnp.float32)
    zero = jnp.zeros((SUB, LANES), jnp.float32)

    def add(total, index, parts):
        hit = small == jnp.broadcast_to(index >> 7, small.shape)
        data = jnp.concatenate([jnp.where(hit, wide(part), zero) for part in parts], 0)
        hits = jnp.where(tall == jnp.broadcast_to(index & (LANES - 1), tall.shape), 1.0, 0.0)
        return total + lax.dot_general(
            data, hits, (((1,), (1,)), ((), ())), precision=lax.Precision.HIGHEST, preferred_element_type=jnp.float32
        )

    for r in range(SUB):
        total = add(total, first[r : r + 1], [force[q][r : r + 1] for q in range(3)])
        total = add(total, second[r : r + 1], [-force[q][r : r + 1] for q in range(3)])
    valid = (lax.broadcasted_iota(jnp.int32, (1, LANES), 1) & (HALF - 1)) < width
    narrow = lower[0:1]
    for a in range(3):
        down, up = near[2 * a], near[2 * a + 1]
        parts = []
        for q in range(3):
            at = 4 + a
            from_up = eu_ref[up, q, at : at + 1, :] * ep_ref[up, at : at + 1, :]
            from_down = eu_ref[down, q, at : at + 1, :] * ep_ref[down, at : at + 1, :]
            parts.append(jnp.where(valid, jnp.where(narrow, from_up, from_down), 0.0))
        total = add(total, where[a : a + 1, :], parts)
    for q in range(3):
        value = -mass[...] * total[q * SUB : (q + 1) * SUB]
        for r in range(SUB):
            out_disp[q : q + 1, r * LANES : (r + 1) * LANES] = value[r : r + 1]


def domains_near(sizes):
    def far(d, n):
        return min(d, n - d)

    ranked = sorted(
        itertools.product(*(range(n) for n in sizes)), key=lambda r: (sum(far(d, n) for d, n in zip(r, sizes)), r)
    )
    span = [sum(far(d, n) for d, n in zip(r, sizes)) for r in ranked]
    ranked = [r for r, s in zip(ranked, span) if s <= REACH]
    counts = [sum(s <= d for s in span) for d in range(REACH + 1)]
    at = {r: i for i, r in enumerate(ranked)}
    near = []
    for r in ranked:
        for a in range(3):
            for move in (-1, 1):
                to = list(r)
                to[a] = (to[a] + move) % sizes[a]
                near.append(at.get(tuple(to), 0))
    return ranked, counts, near


def per_device(old_pos, new_pos, inv_mass, rest_length, bond_pairs, live, send_index):
    sizes = [lax.axis_size(axis) for axis in AXES]
    nx, ny, nz = sizes
    atoms = old_pos.shape[1]
    width = send_index.shape[1]
    tile = (SUB, LANES)
    mass, rest, alive = (v.reshape(tile) for v in (inv_mass, rest_length, live))
    f32, i32 = jnp.float32, jnp.int32
    shape = jax.ShapeDtypeStruct

    *sent, where = pl.pallas_call(
        sent_kernel,
        out_shape=[shape(tile, f32)] * 3 + [shape(tile, i32)],
        in_specs=[VMEM] * 4,
        out_specs=[VMEM] * 4,
        scratch_shapes=[pltpu.VMEM(tile, i32)],
        name="sent",
    )(old_pos, new_pos, mass, send_index)

    arrived = []
    for axis, n, part in zip(AXES, sizes, sent):
        low = lax.ppermute(part, axis, [(i, (i + 1) % n) for i in range(n)])
        high = low if n == 2 else lax.ppermute(part, axis, [(i, (i - 1) % n) for i in range(n)])
        arrived = arrived + [low, high]

    links = pl.pallas_call(
        functools.partial(link_kernel, width),
        out_shape=shape((3 * SUB, LANES), f32),
        in_specs=[VMEM] * 4,
        out_specs=VMEM,
        scratch_shapes=[pltpu.VMEM(tile, i32), pltpu.VMEM(tile, i32), pltpu.VMEM(tile, f32)],
        cost_estimate=pl.CostEstimate(flops=4_000_000, bytes_accessed=100_000, transcendentals=0),
        name="links",
    )(bond_pairs, live.reshape(1, atoms), alive, where)

    pub = pl.pallas_call(
        functools.partial(node_kernel, width),
        out_shape=shape((FIELDS * SUB, LANES), f32),
        in_specs=[VMEM] * 13,
        out_specs=VMEM,
        scratch_shapes=[pltpu.VMEM(tile, i32), pltpu.VMEM(tile, i32), pltpu.VMEM((3 * SUB, LANES), f32)],
        name="nodes",
    )(old_pos, new_pos, mass, rest, alive, bond_pairs, links, *arrived)

    plane = ny * nz
    gathered = lax.all_to_all(jnp.broadcast_to(pub, (plane,) + pub.shape), ("gy", "gz"), 0, 0)
    parts = [gathered]
    for d in range(1, nx):
        parts.append(lax.ppermute(gathered, "gx", [(i, (i - d) % nx) for i in range(nx)]))

    ranked, counts, near = domains_near(sizes)
    order = sorted(range(len(ranked)), key=lambda i: (ranked[i][0], i))
    split = [sum(r[0] == d for r in ranked) for d in range(nx)]
    dy = jnp.asarray([ranked[i][1] for i in order], i32)
    dz = jnp.asarray([ranked[i][2] for i in order], i32)
    source = (lax.axis_index("gy") + dy) % ny * nz + (lax.axis_index("gz") + dz) % nz
    held = -(-len(ranked) // CHUNK) * CHUNK
    near = near + [0] * (6 * (held - len(ranked)))

    def keep(*lead, kind=f32):
        return pltpu.VMEM(lead + tile, kind)

    disp, mult = pl.pallas_call(
        functools.partial(main_kernel, counts, split, width),
        out_shape=[shape((3, atoms), f32), shape(tile, f32)],
        in_specs=[SMEM] * 3 + [VMEM] * (3 + nx),
        out_specs=[VMEM] * 2,
        scratch_shapes=[
            keep(held, 3), keep(held, 3), keep(held), keep(held), keep(held), keep(held, 2, kind=i32), keep(held, kind=i32),
            keep(held, 3), keep(held, 6), keep(held, 2), keep(held), keep(held), keep(held), keep(held), keep(held), keep(held),
            pltpu.VMEM(tile, i32), pltpu.VMEM(tile, i32),
        ],
        name="solve",
    )(source, jnp.asarray(order, i32), jnp.asarray(near, i32), bond_pairs, mass, where, *parts)
    return disp, mult.reshape(atoms)


def solution(mesh):
    flat = P(AXES)
    rows = P(None, AXES)
    return jax.shard_map(
        per_device,
        mesh=mesh,
        in_specs=(rows, rows, flat, flat, rows, flat, P(AXES, None)),
        out_specs=(rows, flat),
        check_vma=False,
    )
```

```python
import functools
import itertools
import math

import jax
import jax.numpy as jnp
import numpy as np
from jax import lax
from jax.experimental import pallas as pl
from jax.experimental.pallas import tpu as pltpu
from jax.sharding import PartitionSpec as P

ORDER = 4
AXES = ("gx", "gy", "gz")
LANES = 128
HALF = LANES // 2
SUB = 8
CHUNK = 16
LOAD = 4
FIELDS = 12
REACH = 2 * (ORDER + 1)
VMEM = pl.BlockSpec(memory_space=pltpu.VMEM)
SMEM = pl.BlockSpec(memory_space=pltpu.SMEM)


def wide(row):
    return jnp.broadcast_to(row, (SUB, LANES))


def pick(tables, row, lane):
    total = jnp.zeros((SUB, LANES), jnp.float32)
    for number, load in tables.items():
        got = jnp.take_along_axis(wide(load()), lane, axis=1, mode="promise_in_bounds")
        total = jnp.where(row == number, got.astype(jnp.float32), total)
    return total


def flat_rows(ref, q):
    return {r: functools.partial(lambda q, r: ref[q : q + 1, r * LANES : (r + 1) * LANES], q, r) for r in range(SUB)}


def tile_rows(ref, base=0):
    return {r: functools.partial(lambda r: ref[base + r : base + r + 1, :], r) for r in range(SUB)}


def stack_rows(ref, q, hold):
    for r in range(SUB):
        hold[r : r + 1, :] = ref[q : q + 1, r * LANES : (r + 1) * LANES]
    return hold[...]


def sent_kernel(old, new, mass, send, out_x, out_y, out_z, where, pad):
    width = send.shape[1]
    pad[...] = jnp.zeros_like(pad)
    pad[0:6, 0:width] = send[...]
    low = pad[...]
    high = pltpu.roll(low, HALF, 1)
    where[...] = jnp.zeros_like(where)
    for a in range(3):
        where[a : a + 1, :] = low[2 * a : 2 * a + 1] + high[2 * a + 1 : 2 * a + 2]
    index = where[...]
    row, lane = index >> 7, index & (LANES - 1)
    tables = [flat_rows(old, q) for q in range(3)] + [flat_rows(new, q) for q in range(3)] + [tile_rows(mass)]
    outs = (out_x, out_y, out_z)
    for a in range(3):
        outs[a][...] = jnp.zeros_like(outs[a])
    for f, table in enumerate(tables):
        got = pick(table, row, lane)
        for a in range(3):
            outs[a][f : f + 1, :] = got[a : a + 1, :]


def second_place(second, width):
    atoms = SUB * LANES
    slot = second - atoms
    block = jnp.zeros_like(second)
    for b in range(1, 6):
        block = block + (slot >= b * width).astype(jnp.int32)
    lane = slot - block * width + (block & 1) * HALF
    remote = second >= atoms
    row = jnp.where(remote, 12 + (block >> 1), second >> 7)
    return row, jnp.where(remote, lane, second & (LANES - 1))


def nt_dot(a, b):
    return lax.dot_general(a, b, (((1,), (1,)), ((), ())), preferred_element_type=jnp.float32)


def split_codes(hit, code):
    code = jnp.broadcast_to(code, hit.shape)
    zero = jnp.zeros_like(code)
    both = jnp.concatenate([jnp.where(hit, code >> 4, zero), jnp.where(hit, code & 15, zero)], 0)
    return both.astype(jnp.float32).astype(jnp.bfloat16)


def lane_hits(lane, count):
    hits = lax.broadcasted_iota(jnp.int32, (LANES, count), 0) == jnp.broadcast_to(lane, (LANES, count))
    return jnp.where(hits, 1.0, 0.0).astype(jnp.bfloat16)


def link_kernel(width, bonds, live_row, live, where, links, hold_a, hold_b, s_ref):
    atoms = SUB * LANES
    first_row = bonds[0:1, :]
    second_row = bonds[1:2, :]
    usable = (live_row[...] != 0) & (first_row != second_row)
    node = lax.broadcasted_iota(jnp.int32, (1, atoms), 1)
    targets = lax.broadcasted_iota(jnp.int32, (2 * SUB, atoms), 0)
    total = jnp.zeros((4 * SUB, LANES), jnp.float32)
    places = ((first_row >> 7, first_row & (LANES - 1)), second_place(second_row, width))
    for end, (row, lane) in enumerate(places):
        row = jnp.where(usable, row, -1)
        hit = targets == jnp.broadcast_to(row, targets.shape)
        total = total + nt_dot(split_codes(hit, 2 * node + end + 1), lane_hits(lane, atoms))
    sums = 16.0 * total[: 2 * SUB] + total[2 * SUB :]

    index = where[...]
    lanes = lax.broadcasted_iota(jnp.int32, (1, LANES), 1)
    valid = ((lanes & (HALF - 1)) < width)
    small = lax.broadcasted_iota(jnp.int32, (SUB, LANES), 0)
    slots = jnp.zeros((2 * SUB, LANES), jnp.float32)
    for a in range(3):
        one = index[a : a + 1, :]
        row = jnp.where(valid, one >> 7, -1)
        hit = small == jnp.broadcast_to(row, small.shape)
        slots = slots + nt_dot(split_codes(hit, (SUB + a) * LANES + lanes + 1), lane_hits(one & (LANES - 1), LANES))
    sent_slot = 16.0 * slots[:SUB] + slots[SUB:]
    s_ref[0:SUB, :] = 4096.0 * sums[:SUB] + sent_slot
    out_code = sums[SUB:]

    first = stack_rows(bonds, 0, hold_a)
    second = stack_rows(bonds, 1, hold_b)
    alive = (live[...] != 0) & (first != second)
    me = lax.broadcasted_iota(jnp.int32, (SUB, LANES), 0) * LANES + lax.broadcasted_iota(jnp.int32, (SUB, LANES), 1)
    none = 2 * (2 * atoms - 1)
    table = tile_rows(s_ref)
    srow, slane = second_place(second, width)
    for end, (row, lane) in enumerate(((first >> 7, first & (LANES - 1)), (srow, slane))):
        both = pick(table, row, lane).astype(jnp.int32)
        code = (both >> 12) - (2 * me + end + 1)
        ghost = both & 4095
        link = jnp.where(code > 0, code - 1, jnp.where(ghost > 0, 2 * (ghost - 1), none))
        if end == 1:
            link = jnp.where(row >= SUB, 2 * (row * LANES + lane), link)
        links[end * SUB : (end + 1) * SUB, :] = jnp.where(alive, link, none).astype(jnp.float32)
    sent = pick(table, index >> 7, index & (LANES - 1)).astype(jnp.int32) >> 12
    sublane = lax.broadcasted_iota(jnp.int32, (SUB, LANES), 0)
    in_row = (sublane < 3) & ((lax.broadcasted_iota(jnp.int32, (SUB, LANES), 1) & (HALF - 1)) < width)
    ends = jnp.where(in_row, sent - 1, jnp.where(sublane >= 4, out_code.astype(jnp.int32) - 1, -1))
    links[2 * SUB : 3 * SUB, :] = ends.astype(jnp.float32)


def node_kernel(width, old, new, mass, rest, live, bonds, links, *refs):
    arrived = refs[:6]
    pub, hold_a, hold_b, got_ref = refs[6:]
    first = stack_rows(bonds, 0, hold_a)
    second = stack_rows(bonds, 1, hold_b)
    lower = lax.broadcasted_iota(jnp.int32, (1, LANES), 1) < HALF
    for a in range(3):
        got_ref[a * SUB : (a + 1) * SUB, :] = jnp.where(lower, arrived[2 * a][...], arrived[2 * a + 1][...])
    row, lane = first >> 7, first & (LANES - 1)
    srow, slane = second_place(second, width)
    tables = [flat_rows(old, q) for q in range(3)] + [flat_rows(new, q) for q in range(3)] + [tile_rows(mass)]
    firsts, seconds = [], []
    for f, table in enumerate(tables):
        firsts.append(pick(table, row, lane))
        more = dict(table)
        for a in range(3):
            more[12 + a] = functools.partial(lambda at: got_ref[at : at + 1, :], a * SUB + f)
        seconds.append(pick(more, srow, slane))
    span = [x - y for x, y in zip(firsts, seconds)]
    alive = live[...].astype(jnp.float32)
    scaling = alive * lax.rsqrt(firsts[6] + seconds[6])
    norm = lax.rsqrt(span[0] * span[0] + span[1] * span[1] + span[2] * span[2] + 0.25)
    values = [scaling * norm * span[q] for q in range(3)]
    values = values + [scaling * span[3 + q] for q in range(3)]
    values = values + [scaling * rest[...], firsts[6], seconds[6]]
    for f, value in enumerate(values):
        pub[f * SUB : (f + 1) * SUB, :] = value
    pub[9 * SUB : 12 * SUB, :] = links[...]


def place(dart):
    return dart >> 8, (dart >> 1) & (LANES - 1)


def main_kernel(
    counts, split, width, source, slot, near, bonds, mass, where, *refs
):
    shifts = len(split)
    pubs = refs[:shifts]
    (
        out_disp, out_mult, u_ref, n_ref, rho_ref, mf_ref, mg_ref, p_ref, e_ref,
        eu_ref, g_ref, w_ref, diag_ref, xa, xb, one_ref, two_ref, ep_ref, hold_a, hold_b,
    ) = refs[shifts:]

    start = 0
    for shift in range(shifts):
        pub = pubs[shift]

        def load(j, pub=pub):
            s = source[j]
            d = slot[j]
            field = [pub[s, f * SUB : (f + 1) * SUB, :] for f in range(FIELDS)]
            u, n = field[0:3], field[3:6]
            both = field[7] + field[8]
            root = both * lax.rsqrt(both)
            size = u[0] * u[0] + u[1] * u[1] + u[2] * u[2]
            dot = u[0] * n[0] + u[1] * n[1] + u[2] * n[2]
            value = dot * root - field[6]
            dart = field[11].astype(jnp.int32)
            row, lane = place(dart)
            sign = jnp.where((dart & 1) == 1, -1.0, 1.0)
            ends = []
            for q in range(3):
                table = {r: functools.partial(lambda q, r: pub[s, q * SUB + r : q * SUB + r + 1, :], q, r) for r in range(SUB)}
                ends.append(sign * pick(table, row, lane))

            def finish():
                diag_ref[d] = 1.0 - both * size
                xa[d] = value
                one_ref[d] = value
                for q in range(3):
                    u_ref[d, q] = u[q]
                    n_ref[d, q] = n[q]
                    eu_ref[d, q] = ends[q]
                rho_ref[d] = field[6]
                mf_ref[d] = field[7]
                mg_ref[d] = field[8]
                p_ref[d, 0] = field[9].astype(jnp.int32)
                p_ref[d, 1] = field[10].astype(jnp.int32)
                e_ref[d] = dart

            return finish

        unroll = math.gcd(LOAD, split[shift])

        def loads(c, carry, load=load, start=start, unroll=unroll):
            for finish in [load(start + c * unroll + k) for k in range(unroll)]:
                finish()
            return carry

        lax.fori_loop(0, split[shift] // unroll, loads, 0)
        start = start + split[shift]

    lower = lax.broadcasted_iota(jnp.int32, (SUB, LANES), 1) < HALF

    def chunks(count, body):
        steps = -(-count // CHUNK)

        def step(c, carry):
            done = [body(c * CHUNK + k) for k in range(CHUNK)]
            for finish in done:
                finish()
            return carry

        if steps == 1:
            step(0, 0)
        else:
            lax.fori_loop(0, steps, step, 0)

    def table_of(i, own, ghost):
        rows = {r: functools.partial(own, i, r) for r in range(SUB)}
        for a in range(3):
            down, up = near[6 * i + 2 * a], near[6 * i + 2 * a + 1]

            def into(a=a, down=down, up=up):
                return jnp.where(lower, wide(ghost(up, 4 + a)), wide(ghost(down, 4 + a)))

            def away(a=a, down=down, up=up):
                return jnp.where(lower, wide(ghost(down, a)), wide(ghost(up, a)))

            rows[SUB + a] = into
            rows[SUB + 4 + a] = away
        return rows

    def pick_ends(i, tables):
        loaded = [{number: wide(make()) for number, make in table.items()} for table in tables]
        results = []
        for end in range(2):
            row, lane = place(p_ref[i, end])
            seen = [number for number in loaded[0] if end == 1 or number < SUB + 4]
            hits = {number: row == number for number in seen}
            got = []
            for data in loaded:
                total = jnp.zeros((SUB, LANES), jnp.float32)
                for number in seen:
                    value = jnp.take_along_axis(data[number], lane, axis=1, mode="promise_in_bounds")
                    total = jnp.where(hits[number], value, total)
                got.append(total)
            results.append(got)
        return results

    def pick_two(i, own, ghost):
        one, two = pick_ends(i, [table_of(i, own, ghost)])
        return one[0], two[0]

    def couple_setup(i):
        u = [u_ref[i, q] for q in range(3)]
        mf, mg = mf_ref[i], mg_ref[i]
        signs = [mf * jnp.where((p_ref[i, 0] & 1) == 1, -1.0, 1.0), -mg * jnp.where((p_ref[i, 1] & 1) == 1, -1.0, 1.0)]
        weights = [jnp.zeros((SUB, LANES), jnp.float32)] * 2
        pulls = []
        tables = [
            table_of(i, lambda i, r, q=q: u_ref[i, q, r : r + 1, :], lambda i, r, q=q: eu_ref[i, q, r : r + 1, :])
            for q in range(3)
        ]
        for end, got in enumerate(pick_ends(i, tables)):
            for q in range(3):
                pull = signs[end] * got[q]
                weights[end] = weights[end] + u[q] * pull
                pulls.append((end * 3 + q, pull))

        def finish():
            for at, pull in pulls:
                g_ref[i, at] = pull
            for end in range(2):
                w_ref[i, end] = weights[end]

        return finish

    chunks(counts[REACH - 1], couple_setup)

    def send_ends(x, count):
        def body(i):
            row, lane = place(e_ref[i])
            got = pick({r: functools.partial(lambda r: x[i, r : r + 1, :], r) for r in range(SUB)}, row, lane)

            def finish():
                ep_ref[i] = got

            return finish

        chunks(count, body)

    def own_of(x):
        return lambda i, r: x[i, r : r + 1, :]

    def ghost_value(i, r):
        return ep_ref[i, r : r + 1, :]

    def expand(current, following, total, reach):
        for term in range(ORDER):
            send_ends(current, counts[reach - term])

            def body(i, current=current, following=following):
                got = pick_two(i, own_of(current), ghost_value)
                value = diag_ref[i] * current[i] - w_ref[i, 0] * got[0] - w_ref[i, 1] * got[1]

                def finish():
                    following[i] = value
                    total[i] = total[i] + value

                return finish

            chunks(counts[reach - term - 1], body)
            current, following = following, current

    expand(xa, xb, one_ref, REACH)
    send_ends(one_ref, counts[ORDER + 2])

    def correct(i):
        got = pick_two(i, own_of(one_ref), ghost_value)
        both = mf_ref[i] + mg_ref[i]
        scaling = lax.rsqrt(both)
        mine = both * one_ref[i]
        length = jnp.zeros((SUB, LANES), jnp.float32)
        for q in range(3):
            part = n_ref[i, q] - scaling * (u_ref[i, q] * mine + g_ref[i, q] * got[0] + g_ref[i, 3 + q] * got[1])
            length = length + part * part
        rho = rho_ref[i]
        square = rho * rho
        value = rho - jnp.sqrt(jnp.maximum(2.0 * square - length, 0.25 * square))

        def finish():
            xa[i] = value
            two_ref[i] = value

        return finish

    chunks(counts[ORDER + 1], correct)
    expand(xa, xb, two_ref, ORDER + 1)

    def join(i):
        value = one_ref[i] + two_ref[i]

        def finish():
            xa[i] = value

        return finish

    chunks(counts[1], join)
    send_ends(xa, counts[1])

    multiplier = xa[0]
    out_mult[...] = multiplier
    first = stack_rows(bonds, 0, hold_a)
    second = stack_rows(bonds, 1, hold_b)
    small = lax.broadcasted_iota(jnp.int32, (SUB, LANES), 0)
    tall = lax.broadcasted_iota(jnp.int32, (LANES, LANES), 0)
    force = [u_ref[0, q] * multiplier for q in range(3)]
    total = jnp.zeros((3 * SUB, LANES), jnp.float32)
    zero = jnp.zeros((SUB, LANES), jnp.float32)

    def add(total, index, parts):
        hit = small == jnp.broadcast_to(index >> 7, small.shape)
        data = jnp.concatenate([jnp.where(hit, wide(part), zero) for part in parts], 0)
        hits = jnp.where(tall == jnp.broadcast_to(index & (LANES - 1), tall.shape), 1.0, 0.0)
        return total + lax.dot_general(
            data, hits, (((1,), (1,)), ((), ())), precision=lax.Precision.HIGHEST, preferred_element_type=jnp.float32
        )

    for r in range(SUB):
        total = add(total, first[r : r + 1], [force[q][r : r + 1] for q in range(3)])
        total = add(total, second[r : r + 1], [-force[q][r : r + 1] for q in range(3)])
    valid = (lax.broadcasted_iota(jnp.int32, (1, LANES), 1) & (HALF - 1)) < width
    narrow = lower[0:1]
    for a in range(3):
        down, up = near[2 * a], near[2 * a + 1]
        parts = []
        for q in range(3):
            at = 4 + a
            from_up = eu_ref[up, q, at : at + 1, :] * ep_ref[up, at : at + 1, :]
            from_down = eu_ref[down, q, at : at + 1, :] * ep_ref[down, at : at + 1, :]
            parts.append(jnp.where(valid, jnp.where(narrow, from_up, from_down), 0.0))
        total = add(total, where[a : a + 1, :], parts)
    for q in range(3):
        value = -mass[...] * total[q * SUB : (q + 1) * SUB]
        for r in range(SUB):
            out_disp[q : q + 1, r * LANES : (r + 1) * LANES] = value[r : r + 1]


def domains_near(sizes):
    def far(d, n):
        return min(d, n - d)

    ranked = sorted(
        itertools.product(*(range(n) for n in sizes)), key=lambda r: (sum(far(d, n) for d, n in zip(r, sizes)), r)
    )
    span = [sum(far(d, n) for d, n in zip(r, sizes)) for r in ranked]
    ranked = [r for r, s in zip(ranked, span) if s <= REACH]
    counts = [sum(s <= d for s in span) for d in range(REACH + 1)]
    at = {r: i for i, r in enumerate(ranked)}
    near = []
    for r in ranked:
        for a in range(3):
            for move in (-1, 1):
                to = list(r)
                to[a] = (to[a] + move) % sizes[a]
                near.append(at.get(tuple(to), 0))
    return ranked, counts, near


def per_device(old_pos, new_pos, inv_mass, rest_length, bond_pairs, live, send_index):
    sizes = [lax.axis_size(axis) for axis in AXES]
    nx, ny, nz = sizes
    atoms = old_pos.shape[1]
    width = send_index.shape[1]
    tile = (SUB, LANES)
    mass, rest, alive = (v.reshape(tile) for v in (inv_mass, rest_length, live))
    f32, i32 = jnp.float32, jnp.int32
    shape = jax.ShapeDtypeStruct

    *sent, where = pl.pallas_call(
        sent_kernel,
        out_shape=[shape(tile, f32)] * 3 + [shape(tile, i32)],
        in_specs=[VMEM] * 4,
        out_specs=[VMEM] * 4,
        scratch_shapes=[pltpu.VMEM(tile, i32)],
        name="sent",
    )(old_pos, new_pos, mass, send_index)

    arrived = []
    for axis, n, part in zip(AXES, sizes, sent):
        low = lax.ppermute(part, axis, [(i, (i + 1) % n) for i in range(n)])
        high = low if n == 2 else lax.ppermute(part, axis, [(i, (i - 1) % n) for i in range(n)])
        arrived = arrived + [low, high]

    links = pl.pallas_call(
        functools.partial(link_kernel, width),
        out_shape=shape((3 * SUB, LANES), f32),
        in_specs=[VMEM] * 4,
        out_specs=VMEM,
        scratch_shapes=[pltpu.VMEM(tile, i32), pltpu.VMEM(tile, i32), pltpu.VMEM(tile, f32)],
        cost_estimate=pl.CostEstimate(flops=4_000_000, bytes_accessed=100_000, transcendentals=0),
        name="links",
    )(bond_pairs, live.reshape(1, atoms), alive, where)

    pub = pl.pallas_call(
        functools.partial(node_kernel, width),
        out_shape=shape((FIELDS * SUB, LANES), f32),
        in_specs=[VMEM] * 13,
        out_specs=VMEM,
        scratch_shapes=[pltpu.VMEM(tile, i32), pltpu.VMEM(tile, i32), pltpu.VMEM((3 * SUB, LANES), f32)],
        name="nodes",
    )(old_pos, new_pos, mass, rest, alive, bond_pairs, links, *arrived)

    plane = ny * nz
    gathered = lax.all_to_all(jnp.broadcast_to(pub, (plane,) + pub.shape), ("gy", "gz"), 0, 0)
    parts = [gathered]
    for d in range(1, nx):
        parts.append(lax.ppermute(gathered, "gx", [(i, (i - d) % nx) for i in range(nx)]))

    ranked, counts, near = domains_near(sizes)
    order = sorted(range(len(ranked)), key=lambda i: (ranked[i][0], i))
    split = [sum(r[0] == d for r in ranked) for d in range(nx)]
    dy = jnp.asarray([ranked[i][1] for i in order], i32)
    dz = jnp.asarray([ranked[i][2] for i in order], i32)
    source = (lax.axis_index("gy") + dy) % ny * nz + (lax.axis_index("gz") + dz) % nz
    held = -(-len(ranked) // CHUNK) * CHUNK
    near = near + [0] * (6 * (held - len(ranked)))

    def keep(*lead, kind=f32):
        return pltpu.VMEM(lead + tile, kind)

    disp, mult = pl.pallas_call(
        functools.partial(main_kernel, counts, split, width),
        out_shape=[shape((3, atoms), f32), shape(tile, f32)],
        in_specs=[SMEM] * 3 + [VMEM] * (3 + nx),
        out_specs=[VMEM] * 2,
        scratch_shapes=[
            keep(held, 3), keep(held, 3), keep(held), keep(held), keep(held), keep(held, 2, kind=i32), keep(held, kind=i32),
            keep(held, 3), keep(held, 6), keep(held, 2), keep(held), keep(held), keep(held), keep(held), keep(held), keep(held),
            pltpu.VMEM(tile, i32), pltpu.VMEM(tile, i32),
        ],
        name="solve",
    )(source, jnp.asarray(order, i32), jnp.asarray(near, i32), bond_pairs, mass, where, *parts)
    return disp, mult.reshape(atoms)


def solution(mesh):
    flat = P(AXES)
    rows = P(None, AXES)
    return jax.shard_map(
        per_device,
        mesh=mesh,
        in_specs=(rows, rows, flat, flat, rows, flat, P(AXES, None)),
        out_specs=(rows, flat),
        check_vma=False,
    )
```

```python
import functools
import itertools

import jax
import jax.numpy as jnp
import numpy as np
from jax import lax
from jax.experimental import pallas as pl
from jax.experimental.pallas import tpu as pltpu
from jax.sharding import PartitionSpec as P

ORDER = 4
AXES = ("gx", "gy", "gz")
LANES = 128
HALF = LANES // 2
SUB = 8
CHUNK = 16
LOAD = 4
FIELDS = 12
REACH = 2 * (ORDER + 1)
VMEM = pl.BlockSpec(memory_space=pltpu.VMEM)


def wide(row):
    return jnp.broadcast_to(row, (SUB, LANES))


def pick(tables, row, lane):
    total = jnp.zeros((SUB, LANES), jnp.float32)
    for number, load in tables.items():
        got = jnp.take_along_axis(wide(load()), lane, axis=1, mode="promise_in_bounds")
        total = jnp.where(row == number, got.astype(jnp.float32), total)
    return total


def flat_rows(ref, q):
    return {r: functools.partial(lambda q, r: ref[q : q + 1, r * LANES : (r + 1) * LANES], q, r) for r in range(SUB)}


def tile_rows(ref, base=0):
    return {r: functools.partial(lambda r: ref[base + r : base + r + 1, :], r) for r in range(SUB)}


def stack_rows(ref, q, hold):
    for r in range(SUB):
        hold[r : r + 1, :] = ref[q : q + 1, r * LANES : (r + 1) * LANES]
    return hold[...]


def second_place(second, width):
    atoms = SUB * LANES
    slot = second - atoms
    block = jnp.zeros_like(second)
    for b in range(1, 6):
        block = block + (slot >= b * width).astype(jnp.int32)
    lane = slot - block * width + (block & 1) * HALF
    remote = second >= atoms
    row = jnp.where(remote, 12 + (block >> 1), second >> 7)
    return row, jnp.where(remote, lane, second & (LANES - 1))


def nt_dot(a, b):
    return lax.dot_general(a, b, (((1,), (1,)), ((), ())), preferred_element_type=jnp.float32)


def split_codes(hit, code):
    code = jnp.broadcast_to(code, hit.shape)
    zero = jnp.zeros_like(code)
    both = jnp.concatenate([jnp.where(hit, code >> 4, zero), jnp.where(hit, code & 15, zero)], 0)
    return both.astype(jnp.float32).astype(jnp.bfloat16)


def lane_hits(lane, count):
    hits = lax.broadcasted_iota(jnp.int32, (LANES, count), 0) == jnp.broadcast_to(lane, (LANES, count))
    return jnp.where(hits, 1.0, 0.0).astype(jnp.bfloat16)


def publish_kernel(width, old, new, mass, rest, live, live_row, bonds, send, pub, own, pad, hold_a, hold_b, s_ref, row_ref):
    atoms = SUB * LANES
    sublane = lax.broadcasted_iota(jnp.int32, (SUB, LANES), 0)
    spot = lax.broadcasted_iota(jnp.int32, (SUB, LANES), 1)
    lanes = spot[0:1]

    pad[...] = jnp.zeros_like(pad)
    pad[0:6, 0:width] = send[...]
    low = pad[...]
    high = pltpu.roll(low, HALF, 1)
    ones = [low[2 * a : 2 * a + 1] + high[2 * a + 1 : 2 * a + 2] for a in range(3)]
    for a in range(3):
        pad[a : a + 1, :] = ones[a]
    index = pad[...]
    index = jnp.where(sublane < 3, index, 0)
    sent_place = (index >> 7, index & (LANES - 1))

    first_row = bonds[0:1, :]
    second_row = bonds[1:2, :]
    usable = (live_row[...] != 0) & (first_row != second_row)
    node = lax.broadcasted_iota(jnp.int32, (1, atoms), 1)
    targets = lax.broadcasted_iota(jnp.int32, (2 * SUB, atoms), 0)
    total = jnp.zeros((4 * SUB, LANES), jnp.float32)
    places = ((first_row >> 7, first_row & (LANES - 1)), second_place(second_row, width))
    marks = []
    for end, (row, lane) in enumerate(places):
        row = jnp.where(usable, row, -1)
        hits = lane_hits(lane, atoms)
        marks.append((row, hits))
        hit = targets == jnp.broadcast_to(row, targets.shape)
        total = total + nt_dot(split_codes(hit, 2 * node + end + 1), hits)
    sums = 16.0 * total[: 2 * SUB] + total[2 * SUB :]

    valid = (lanes & (HALF - 1)) < width
    slots = jnp.zeros((2 * SUB, LANES), jnp.float32)
    for a in range(3):
        row = jnp.where(valid, ones[a] >> 7, -1)
        hit = sublane == jnp.broadcast_to(row, sublane.shape)
        slots = slots + nt_dot(split_codes(hit, (SUB + a) * LANES + lanes + 1), lane_hits(ones[a] & (LANES - 1), LANES))
    sent_slot = 16.0 * slots[:SUB] + slots[SUB:]
    s_ref[0:SUB, :] = 4096.0 * sums[:SUB] + sent_slot
    out_code = sums[SUB:]

    first = stack_rows(bonds, 0, hold_a)
    second = stack_rows(bonds, 1, hold_b)
    alive = (live[...] != 0) & (first != second)
    me = sublane * LANES + spot
    none = 2 * (2 * atoms - 1)
    table = tile_rows(s_ref)
    ends = ((first >> 7, first & (LANES - 1)), second_place(second, width))
    base = 9 * SUB
    for end, (row, lane) in enumerate(ends):
        both = pick(table, row, lane).astype(jnp.int32)
        code = (both >> 12) - (2 * me + end + 1)
        ghost = both & 4095
        link = jnp.where(code > 0, code - 1, jnp.where(ghost > 0, 2 * (ghost - 1), none))
        if end == 1:
            link = jnp.where(row >= SUB, 2 * (row * LANES + lane), link)
        pub[base + end * SUB : base + (end + 1) * SUB, :] = jnp.where(alive, link, none).astype(jnp.float32)
        lead = jnp.where(alive & (2 * me + end + 1 > code), 1, 0)
        for r in range(SUB):
            row_ref[end : end + 1, r * LANES : (r + 1) * LANES] = lead[r : r + 1]
    sent = pick(table, *sent_place).astype(jnp.int32) >> 12
    in_row = (sublane < 3) & ((spot & (HALF - 1)) < width)
    darts = jnp.where(in_row, sent - 1, jnp.where(sublane >= 4, out_code.astype(jnp.int32) - 1, -1))
    pub[base + 2 * SUB : base + 3 * SUB, :] = darts.astype(jnp.float32)

    total = jnp.zeros((2 * SUB, LANES), jnp.float32)
    for end, (row, hits) in enumerate(marks):
        row = jnp.where(row_ref[end : end + 1, :] != 0, row, -1)
        hit = targets[:SUB] == jnp.broadcast_to(row, (SUB, atoms))
        total = total + nt_dot(split_codes(hit, 2 * node + end + 1), hits)
    lead = 16.0 * total[:SUB] + total[SUB:]
    own[0:SUB, :] = lead.astype(jnp.int32) - 1
    own[SUB : 2 * SUB, :] = (sums[:SUB] - lead).astype(jnp.int32) - 1
    own[2 * SUB : 3 * SUB, :] = sent_slot.astype(jnp.int32) - 1

    tables = [flat_rows(old, q) for q in range(3)] + [flat_rows(new, q) for q in range(3)] + [tile_rows(mass)]
    firsts, seconds = [], []
    for f, table in enumerate(tables):
        firsts.append(pick(table, *ends[0]))
        seconds.append(pick(table, *ends[1]))
        got = pick(table, *sent_place)
        at = FIELDS * SUB + 3 * f
        pub[at : at + 3, :] = got[0:3]
    pub[FIELDS * SUB + 21 : FIELDS * SUB + 24, :] = jnp.zeros((3, LANES), jnp.float32)
    weight = live[...].astype(jnp.float32)
    away = ends[1][0] >= SUB
    span = [weight * (x - y) for x, y in zip(firsts, seconds)]
    scaling = jnp.where(away, 1.0, lax.rsqrt(firsts[6] + seconds[6]))
    norm = jnp.where(away, 1.0, lax.rsqrt(span[0] * span[0] + span[1] * span[1] + span[2] * span[2] + 0.25))
    values = [scaling * norm * span[q] for q in range(3)]
    values = values + [scaling * span[3 + q] for q in range(3)]
    values = values + [scaling * weight * rest[...], firsts[6], seconds[6]]
    for f, value in enumerate(values):
        pub[f * SUB : (f + 1) * SUB, :] = value


def place(dart):
    return dart >> 8, (dart >> 1) & (LANES - 1)


def main_kernel(sizes, ranked, counts, near_list, mass, own, *refs):
    nx, ny, nz = sizes
    pubs = refs[:nx]
    (
        out_disp, out_mult, u_ref, n_ref, rho_ref, mf_ref, mg_ref, p_ref, e_ref,
        eu_ref, g_ref, w_ref, diag_ref, xa, xb, one_ref, two_ref, ep_ref, near,
    ) = refs[nx:]
    here = (lax.axis_index("gy"), lax.axis_index("gz"))
    for at, value in enumerate(near_list):
        near[at] = value
    lower = lax.broadcasted_iota(jnp.int32, (SUB, LANES), 1) < HALF

    def wrap(value, n):
        value = jnp.where(value >= n, value - n, value)
        return jnp.where(value < 0, value + n, value)

    def source(relative):
        dx, dy, dz = (d % n for d, n in zip(relative, sizes))
        return pubs[dx], wrap(here[0] + dy, ny) * nz + wrap(here[1] + dz, nz)

    def load(d):
        pub, s = source(ranked[d])
        field = [pub[s, f * SUB : (f + 1) * SUB, :] for f in range(FIELDS)]
        row, lane = place(field[10].astype(jnp.int32))
        away = (row >= 12) & (row < 15)
        beside = []
        for a in range(3):
            for move in (-1, 1):
                to = list(ranked[d])
                to[a] += move
                beside.append(source(to))
        remote = []
        for f in range(7):
            rows = {}
            for a in range(3):
                at = FIELDS * SUB + 3 * f + a

                def make(a=a, at=at):
                    (down, i), (up, j) = beside[2 * a], beside[2 * a + 1]
                    return jnp.where(lower, wide(down[i, at : at + 1, :]), wide(up[j, at : at + 1, :]))

                rows[12 + a] = make
            remote.append(pick(rows, row, lane))
        span = [field[q] - remote[q] for q in range(6)]
        mf = field[7]
        mg = jnp.where(away, remote[6], field[8])
        both = mf + mg
        scaling = lax.rsqrt(both)
        norm = scaling * lax.rsqrt(span[0] * span[0] + span[1] * span[1] + span[2] * span[2] + 0.25)
        u = [jnp.where(away, norm * span[q], field[q]) for q in range(3)]
        n = [jnp.where(away, scaling * span[3 + q], field[3 + q]) for q in range(3)]
        rho = jnp.where(away, scaling * field[6], field[6])
        root = both * scaling
        size = u[0] * u[0] + u[1] * u[1] + u[2] * u[2]
        dot = u[0] * n[0] + u[1] * n[1] + u[2] * n[2]
        value = dot * root - rho

        def finish():
            diag_ref[d] = 1.0 - both * size
            xa[d] = value
            one_ref[d] = value
            for q in range(3):
                u_ref[d, q] = u[q]
                n_ref[d, q] = n[q]
            rho_ref[d] = rho
            mf_ref[d] = mf
            mg_ref[d] = mg
            p_ref[d, 0] = field[9].astype(jnp.int32)
            p_ref[d, 1] = field[10].astype(jnp.int32)
            e_ref[d] = field[11].astype(jnp.int32)

        return finish

    for c in range(0, len(ranked), LOAD):
        done = [load(d) for d in range(c, min(c + LOAD, len(ranked)))]
        for finish in done:
            finish()

    def chunks(count, body):
        steps = -(-count // CHUNK)

        def step(c, carry):
            done = [body(c * CHUNK + k) for k in range(CHUNK)]
            for finish in done:
                finish()
            return carry

        if steps == 1:
            step(0, 0)
        else:
            lax.fori_loop(0, steps, step, 0)

    def table_of(i, own, ghost):
        rows = {r: functools.partial(own, i, r) for r in range(SUB)}
        for a in range(3):
            down, up = near[6 * i + 2 * a], near[6 * i + 2 * a + 1]

            def into(a=a, down=down, up=up):
                return jnp.where(lower, wide(ghost(up, 4 + a)), wide(ghost(down, 4 + a)))

            def away(a=a, down=down, up=up):
                return jnp.where(lower, wide(ghost(down, a)), wide(ghost(up, a)))

            rows[SUB + a] = into
            rows[SUB + 4 + a] = away
        return rows

    def pick_ends(i, tables):
        loaded = [{number: wide(make()) for number, make in table.items()} for table in tables]
        results = []
        for end in range(2):
            row, lane = place(p_ref[i, end])
            seen = [number for number in loaded[0] if end == 1 or number < SUB + 4]
            hits = {number: row == number for number in seen}
            got = []
            for data in loaded:
                total = jnp.zeros((SUB, LANES), jnp.float32)
                for number in seen:
                    value = jnp.take_along_axis(data[number], lane, axis=1, mode="promise_in_bounds")
                    total = jnp.where(hits[number], value, total)
                got.append(total)
            results.append(got)
        return results

    def pick_two(i, own, ghost):
        one, two = pick_ends(i, [table_of(i, own, ghost)])
        return one[0], two[0]

    def couple_setup(i):
        u = [u_ref[i, q] for q in range(3)]
        mf, mg = mf_ref[i], mg_ref[i]
        signs = [mf * jnp.where((p_ref[i, 0] & 1) == 1, -1.0, 1.0), -mg * jnp.where((p_ref[i, 1] & 1) == 1, -1.0, 1.0)]
        weights = [jnp.zeros((SUB, LANES), jnp.float32)] * 2
        pulls = []
        tables = [
            table_of(i, lambda i, r, q=q: u_ref[i, q, r : r + 1, :], lambda i, r, q=q: eu_ref[i, q, r : r + 1, :])
            for q in range(3)
        ]
        for end, got in enumerate(pick_ends(i, tables)):
            for q in range(3):
                pull = signs[end] * got[q]
                weights[end] = weights[end] + u[q] * pull
                pulls.append((end * 3 + q, pull))

        def finish():
            for at, pull in pulls:
                g_ref[i, at] = pull
            for end in range(2):
                w_ref[i, end] = weights[end]

        return finish

    def unit_ends(i):
        dart = e_ref[i]
        row, lane = place(dart)
        sign = jnp.where((dart & 1) == 1, -1.0, 1.0)
        ends = [
            sign * pick({r: functools.partial(lambda q, r: u_ref[i, q, r : r + 1, :], q, r) for r in range(SUB)}, row, lane)
            for q in range(3)
        ]

        def finish():
            for q in range(3):
                eu_ref[i, q] = ends[q]

        return finish

    chunks(counts[REACH], unit_ends)
    chunks(counts[REACH - 1], couple_setup)

    def send_ends(x, count):
        def body(i):
            row, lane = place(e_ref[i])
            got = pick({r: functools.partial(lambda r: x[i, r : r + 1, :], r) for r in range(SUB)}, row, lane)

            def finish():
                ep_ref[i] = got

            return finish

        chunks(count, body)

    def own_of(x):
        return lambda i, r: x[i, r : r + 1, :]

    def ghost_value(i, r):
        return ep_ref[i, r : r + 1, :]

    def expand(current, following, total, reach):
        for term in range(ORDER):
            send_ends(current, counts[reach - term])

            def body(i, current=current, following=following):
                got = pick_two(i, own_of(current), ghost_value)
                value = diag_ref[i] * current[i] - w_ref[i, 0] * got[0] - w_ref[i, 1] * got[1]

                def finish():
                    following[i] = value
                    total[i] = total[i] + value

                return finish

            chunks(counts[reach - term - 1], body)
            current, following = following, current

    expand(xa, xb, one_ref, REACH)
    send_ends(one_ref, counts[ORDER + 2])

    def correct(i):
        got = pick_two(i, own_of(one_ref), ghost_value)
        both = mf_ref[i] + mg_ref[i]
        scaling = lax.rsqrt(both)
        mine = both * one_ref[i]
        length = jnp.zeros((SUB, LANES), jnp.float32)
        for q in range(3):
            part = n_ref[i, q] - scaling * (u_ref[i, q] * mine + g_ref[i, q] * got[0] + g_ref[i, 3 + q] * got[1])
            length = length + part * part
        rho = rho_ref[i]
        square = rho * rho
        value = rho - jnp.sqrt(jnp.maximum(2.0 * square - length, 0.25 * square))

        def finish():
            xa[i] = value
            two_ref[i] = value

        return finish

    chunks(counts[ORDER + 1], correct)
    expand(xa, xb, two_ref, ORDER + 1)

    def join(i):
        value = one_ref[i] + two_ref[i]

        def finish():
            xa[i] = value

        return finish

    chunks(counts[1], join)
    send_ends(xa, counts[1])

    multiplier = xa[0]
    out_mult[...] = multiplier
    for q in range(3):
        xb[q] = u_ref[0, q] * multiplier
    narrow = lower[0:1]
    total = [jnp.zeros((SUB, LANES), jnp.float32)] * 3
    for end in range(2):
        dart = own[end * SUB : (end + 1) * SUB, :]
        row, lane = place(dart)
        sign = jnp.where((dart & 1) == 1, -1.0, 1.0)
        for q in range(3):
            rows = {r: functools.partial(lambda q, r: xb[q, r : r + 1, :], q, r) for r in range(SUB)}
            total[q] = total[q] + sign * pick(rows, row, lane)
    ghost = own[2 * SUB : 3 * SUB, :]
    for q in range(3):
        rows = {}
        for a in range(3):

            def make(a=a, q=q):
                down, up = near_list[2 * a], near_list[2 * a + 1]
                at = 4 + a
                from_up = eu_ref[up, q, at : at + 1, :] * ep_ref[up, at : at + 1, :]
                from_down = eu_ref[down, q, at : at + 1, :] * ep_ref[down, at : at + 1, :]
                return jnp.where(narrow, from_up, from_down)

            rows[SUB + a] = make
        value = -mass[...] * (total[q] + pick(rows, ghost >> 7, ghost & (LANES - 1)))
        for r in range(SUB):
            out_disp[q : q + 1, r * LANES : (r + 1) * LANES] = value[r : r + 1]


def domains_near(sizes):
    def far(d, n):
        return min(d, n - d)

    ranked = sorted(
        itertools.product(*(range(n) for n in sizes)), key=lambda r: (sum(far(d, n) for d, n in zip(r, sizes)), r)
    )
    span = [sum(far(d, n) for d, n in zip(r, sizes)) for r in ranked]
    ranked = [r for r, s in zip(ranked, span) if s <= REACH]
    counts = [sum(s <= d for s in span) for d in range(REACH + 1)]
    at = {r: i for i, r in enumerate(ranked)}
    near = []
    for r in ranked:
        for a in range(3):
            for move in (-1, 1):
                to = list(r)
                to[a] = (to[a] + move) % sizes[a]
                near.append(at.get(tuple(to), 0))
    return ranked, counts, near


def per_device(old_pos, new_pos, inv_mass, rest_length, bond_pairs, live, send_index):
    sizes = [lax.axis_size(axis) for axis in AXES]
    nx, ny, nz = sizes
    atoms = old_pos.shape[1]
    width = send_index.shape[1]
    tile = (SUB, LANES)
    mass, rest, alive = (v.reshape(tile) for v in (inv_mass, rest_length, live))
    f32, i32 = jnp.float32, jnp.int32
    shape = jax.ShapeDtypeStruct

    pub, own = pl.pallas_call(
        functools.partial(publish_kernel, width),
        out_shape=[shape((FIELDS * SUB + 24, LANES), f32), shape((3 * SUB, LANES), i32)],
        in_specs=[VMEM] * 8,
        out_specs=[VMEM] * 2,
        scratch_shapes=[pltpu.VMEM(tile, i32)] * 3 + [pltpu.VMEM(tile, f32), pltpu.VMEM((2, atoms), i32)],
        name="publish",
    )(old_pos, new_pos, mass, rest, alive, live.reshape(1, atoms), bond_pairs, send_index)

    plane = ny * nz
    gathered = lax.all_to_all(jnp.broadcast_to(pub, (plane,) + pub.shape), ("gy", "gz"), 0, 0)
    parts = [gathered]
    for d in range(1, nx):
        parts.append(lax.ppermute(gathered, "gx", [(i, (i - d) % nx) for i in range(nx)]))

    ranked, counts, near = domains_near(sizes)
    held = -(-len(ranked) // CHUNK) * CHUNK
    near = near + [0] * (6 * (held - len(ranked)))

    def keep(*lead, kind=f32):
        return pltpu.VMEM(lead + tile, kind)

    disp, mult = pl.pallas_call(
        functools.partial(main_kernel, sizes, ranked, counts, near),
        out_shape=[shape((3, atoms), f32), shape(tile, f32)],
        in_specs=[VMEM] * (2 + nx),
        out_specs=[VMEM] * 2,
        scratch_shapes=[
            keep(held, 3), keep(held, 3), keep(held), keep(held), keep(held), keep(held, 2, kind=i32), keep(held, kind=i32),
            keep(held, 3), keep(held, 6), keep(held, 2), keep(held), keep(held), keep(held), keep(held), keep(held), keep(held),
            pltpu.SMEM((len(near),), i32),
        ],
        name="solve",
    )(mass, own, *parts)
    return disp, mult.reshape(atoms)


def solution(mesh):
    flat = P(AXES)
    rows = P(None, AXES)
    return jax.shard_map(
        per_device,
        mesh=mesh,
        in_specs=(rows, rows, flat, flat, rows, flat, P(AXES, None)),
        out_specs=(rows, flat),
        check_vma=False,
    )
```

```python
import functools
import itertools

import jax
import jax.numpy as jnp
import numpy as np
from jax import lax
from jax.experimental import pallas as pl
from jax.experimental.pallas import tpu as pltpu
from jax.sharding import PartitionSpec as P

ORDER = 4
AXES = ("gx", "gy", "gz")
LANES = 128
HALF = LANES // 2
SUB = 8
CHUNK = 16
LOAD = 4
FIELDS = 11
REACH = 2 * (ORDER + 1)
VMEM = pl.BlockSpec(memory_space=pltpu.VMEM)


def wide(row):
    return jnp.broadcast_to(row, (SUB, LANES))


def pick(tables, row, lane):
    total = jnp.zeros((SUB, LANES), jnp.float32)
    for number, load in tables.items():
        got = jnp.take_along_axis(wide(load()), lane, axis=1, mode="promise_in_bounds")
        total = jnp.where(row == number, got.astype(jnp.float32), total)
    return total


def flat_rows(ref, q):
    return {r: functools.partial(lambda q, r: ref[q : q + 1, r * LANES : (r + 1) * LANES], q, r) for r in range(SUB)}


def tile_rows(ref, base=0):
    return {r: functools.partial(lambda r: ref[base + r : base + r + 1, :], r) for r in range(SUB)}


def stack_rows(ref, q, hold):
    for r in range(SUB):
        hold[r : r + 1, :] = ref[q : q + 1, r * LANES : (r + 1) * LANES]
    return hold[...]


def second_place(second, width):
    atoms = SUB * LANES
    slot = second - atoms
    block = jnp.zeros_like(second)
    for b in range(1, 6):
        block = block + (slot >= b * width).astype(jnp.int32)
    lane = slot - block * width + (block & 1) * HALF
    remote = second >= atoms
    row = jnp.where(remote, 12 + (block >> 1), second >> 7)
    return row, jnp.where(remote, lane, second & (LANES - 1))


def nt_dot(a, b):
    return lax.dot_general(a, b, (((1,), (1,)), ((), ())), preferred_element_type=jnp.float32)


def split_codes(hit, code):
    code = jnp.broadcast_to(code, hit.shape)
    zero = jnp.zeros_like(code)
    both = jnp.concatenate([jnp.where(hit, code >> 4, zero), jnp.where(hit, code & 15, zero)], 0)
    return both.astype(jnp.float32).astype(jnp.bfloat16)


def lane_hits(lane, count):
    hits = lax.broadcasted_iota(jnp.int32, (LANES, count), 0) == jnp.broadcast_to(lane, (LANES, count))
    return jnp.where(hits, 1.0, 0.0).astype(jnp.bfloat16)


def publish_kernel(width, old, new, mass, rest, live, live_row, bonds, send, pub, own, pad, hold_a, hold_b, s_ref, row_ref):
    atoms = SUB * LANES
    sublane = lax.broadcasted_iota(jnp.int32, (SUB, LANES), 0)
    spot = lax.broadcasted_iota(jnp.int32, (SUB, LANES), 1)
    lanes = spot[0:1]

    pad[...] = jnp.zeros_like(pad)
    pad[0:6, 0:width] = send[...]
    low = pad[...]
    high = pltpu.roll(low, HALF, 1)
    ones = [low[2 * a : 2 * a + 1] + high[2 * a + 1 : 2 * a + 2] for a in range(3)]
    for a in range(3):
        pad[a : a + 1, :] = ones[a]
    index = pad[...]
    index = jnp.where(sublane < 3, index, 0)
    sent_place = (index >> 7, index & (LANES - 1))

    first_row = bonds[0:1, :]
    second_row = bonds[1:2, :]
    usable = (live_row[...] != 0) & (first_row != second_row)
    node = lax.broadcasted_iota(jnp.int32, (1, atoms), 1)
    targets = lax.broadcasted_iota(jnp.int32, (2 * SUB, atoms), 0)
    total = jnp.zeros((4 * SUB, LANES), jnp.float32)
    places = ((first_row >> 7, first_row & (LANES - 1)), second_place(second_row, width))
    marks = []
    for end, (row, lane) in enumerate(places):
        row = jnp.where(usable, row, -1)
        hits = lane_hits(lane, atoms)
        marks.append((row, hits))
        hit = targets == jnp.broadcast_to(row, targets.shape)
        total = total + nt_dot(split_codes(hit, 2 * node + end + 1), hits)
    sums = 16.0 * total[: 2 * SUB] + total[2 * SUB :]

    valid = (lanes & (HALF - 1)) < width
    slots = jnp.zeros((2 * SUB, LANES), jnp.float32)
    for a in range(3):
        row = jnp.where(valid, ones[a] >> 7, -1)
        hit = sublane == jnp.broadcast_to(row, sublane.shape)
        slots = slots + nt_dot(split_codes(hit, (SUB + a) * LANES + lanes + 1), lane_hits(ones[a] & (LANES - 1), LANES))
    sent_slot = 16.0 * slots[:SUB] + slots[SUB:]
    s_ref[0:SUB, :] = 4096.0 * sums[:SUB] + sent_slot
    out_code = sums[SUB:]

    first = stack_rows(bonds, 0, hold_a)
    second = stack_rows(bonds, 1, hold_b)
    alive = (live[...] != 0) & (first != second)
    me = sublane * LANES + spot
    none = 2 * (2 * atoms - 1)
    table = tile_rows(s_ref)
    ends = ((first >> 7, first & (LANES - 1)), second_place(second, width))
    base = 9 * SUB
    for end, (row, lane) in enumerate(ends):
        both = pick(table, row, lane).astype(jnp.int32)
        code = (both >> 12) - (2 * me + end + 1)
        ghost = both & 4095
        link = jnp.where(code > 0, code - 1, jnp.where(ghost > 0, 2 * (ghost - 1), none))
        if end == 1:
            link = jnp.where(row >= SUB, 2 * (row * LANES + lane), link)
        pub[base + end * SUB : base + (end + 1) * SUB, :] = jnp.where(alive, link, none).astype(jnp.float32)
        lead = jnp.where(alive & (2 * me + end + 1 > code), 1, 0)
        for r in range(SUB):
            row_ref[end : end + 1, r * LANES : (r + 1) * LANES] = lead[r : r + 1]
    sent = pick(table, *sent_place).astype(jnp.int32) >> 12
    in_row = (sublane < 3) & ((spot & (HALF - 1)) < width)
    darts = jnp.where(in_row, sent - 1, jnp.where(sublane >= 4, out_code.astype(jnp.int32) - 1, -1))
    tail = FIELDS * SUB
    darts = darts.astype(jnp.float32)
    pub[tail : tail + 3, :] = darts[0:3]
    pub[tail + 3 : tail + 6, :] = darts[4:7]

    total = jnp.zeros((2 * SUB, LANES), jnp.float32)
    for end, (row, hits) in enumerate(marks):
        row = jnp.where(row_ref[end : end + 1, :] != 0, row, -1)
        hit = targets[:SUB] == jnp.broadcast_to(row, (SUB, atoms))
        total = total + nt_dot(split_codes(hit, 2 * node + end + 1), hits)
    lead = 16.0 * total[:SUB] + total[SUB:]
    own[0:SUB, :] = lead.astype(jnp.int32) - 1
    own[SUB : 2 * SUB, :] = (sums[:SUB] - lead).astype(jnp.int32) - 1
    own[2 * SUB : 3 * SUB, :] = sent_slot.astype(jnp.int32) - 1

    tables = [flat_rows(old, q) for q in range(3)] + [flat_rows(new, q) for q in range(3)] + [tile_rows(mass)]
    firsts = [pick(table, *ends[0]) for table in tables]
    seconds = [pick(table, *ends[1]) for table in tables]
    heavy = pick(tables[6], *sent_place)
    for f in range(6):
        moved = pltpu.roll(heavy, (width - f * (HALF - width)) % LANES, 1)
        got = jnp.where((spot & (HALF - 1)) < width, pick(tables[f], *sent_place), moved)
        pub[tail + 6 + 3 * f : tail + 9 + 3 * f, :] = got[0:3]
    weight = live[...].astype(jnp.float32)
    away = ends[1][0] >= SUB
    span = [weight * (x - y) for x, y in zip(firsts, seconds)]
    scaling = jnp.where(away, 1.0, lax.rsqrt(firsts[6] + seconds[6]))
    norm = jnp.where(away, 1.0, lax.rsqrt(span[0] * span[0] + span[1] * span[1] + span[2] * span[2] + 0.25))
    values = [scaling * norm * span[q] for q in range(3)]
    values = values + [scaling * span[3 + q] for q in range(3)]
    values = values + [scaling * weight * rest[...], firsts[6], seconds[6]]
    for f, value in enumerate(values):
        pub[f * SUB : (f + 1) * SUB, :] = value


def place(dart):
    return dart >> 8, (dart >> 1) & (LANES - 1)


def main_kernel(sizes, width, ranked, counts, near_list, mass, own, *refs):
    nx, ny, nz = sizes
    pubs = refs[:nx]
    (
        out_disp, out_mult, u_ref, n_ref, rho_ref, mf_ref, mg_ref, p_ref, e_ref,
        eu_ref, g_ref, w_ref, diag_ref, xa, xb, one_ref, two_ref, ea, eb, near,
    ) = refs[nx:]
    here = (lax.axis_index("gy"), lax.axis_index("gz"))
    for at, value in enumerate(near_list):
        near[at] = value
    lower = lax.broadcasted_iota(jnp.int32, (SUB, LANES), 1) < HALF

    def wrap(value, n):
        value = jnp.where(value >= n, value - n, value)
        return jnp.where(value < 0, value + n, value)

    def source(relative):
        dx, dy, dz = (d % n for d, n in zip(relative, sizes))
        return pubs[dx], wrap(here[0] + dy, ny) * nz + wrap(here[1] + dz, nz)

    def ends_of(value, dart):
        row, lane = place(dart)
        return pick({r: functools.partial(lambda r: value(r), r) for r in range(SUB)}, row, lane)

    def load(d):
        pub, s = source(ranked[d])
        field = [pub[s, f * SUB : (f + 1) * SUB, :] for f in range(FIELDS)]
        row, lane = place(field[10].astype(jnp.int32))
        away = (row >= 12) & (row < 15)
        beside = []
        for a in range(3):
            for move in (-1, 1):
                to = list(ranked[d])
                to[a] += move
                beside.append(source(to))
        def sent_row(f, a):
            at = FIELDS * SUB + 6 + 3 * f + a
            (down, i), (up, j) = beside[2 * a], beside[2 * a + 1]
            return jnp.where(lower, wide(down[i, at : at + 1, :]), wide(up[j, at : at + 1, :]))

        sent = {(f, a): sent_row(f, a) for f in range(6) for a in range(3)}
        remote = [pick({12 + a: functools.partial(sent.get, (f, a)) for a in range(3)}, row, lane) for f in range(6)]
        spare = HALF - width
        inner = lane & (HALF - 1)
        piece = sum((inner >= f * spare).astype(jnp.int32) for f in range(1, -(-width // spare)))
        tables = {16 * f + 12 + a: functools.partial(sent.get, (f, a)) for f in range(-(-width // spare)) for a in range(3)}
        remote.append(pick(tables, 16 * piece + row, (lane - inner) + width + inner - piece * spare))
        span = [field[q] - remote[q] for q in range(6)]
        mf = field[7]
        mg = jnp.where(away, remote[6], field[8])
        both = mf + mg
        scaling = lax.rsqrt(both)
        norm = scaling * lax.rsqrt(span[0] * span[0] + span[1] * span[1] + span[2] * span[2] + 0.25)
        u = [jnp.where(away, norm * span[q], field[q]) for q in range(3)]
        n = [jnp.where(away, scaling * span[3 + q], field[3 + q]) for q in range(3)]
        rho = jnp.where(away, scaling * field[6], field[6])
        root = both * scaling
        size = u[0] * u[0] + u[1] * u[1] + u[2] * u[2]
        dot = u[0] * n[0] + u[1] * n[1] + u[2] * n[2]
        value = dot * root - rho
        at = FIELDS * SUB
        darts = [pub[s, at + 3 * h : at + 3 * h + 3, :].astype(jnp.int32) for h in range(2)]

        def finish():
            diag_ref[d] = 1.0 - both * size
            xa[d] = value
            one_ref[d] = value
            for q in range(3):
                u_ref[d, q] = u[q]
                n_ref[d, q] = n[q]
            rho_ref[d] = rho
            mf_ref[d] = mf
            mg_ref[d] = mg
            p_ref[d, 0] = field[9].astype(jnp.int32)
            p_ref[d, 1] = field[10].astype(jnp.int32)
            e_ref[d] = jnp.full((SUB, LANES), -1, jnp.int32)
            e_ref[d, 0:3] = darts[0]
            e_ref[d, 4:7] = darts[1]

        return finish

    def load_ends(d):
        dart = e_ref[d]
        sign = jnp.where((dart & 1) == 1, -1.0, 1.0)
        unit = [sign * ends_of(lambda r, q=q: u_ref[d, q, r : r + 1, :], dart) for q in range(3)]
        ends = ends_of(lambda r: xa[d, r : r + 1, :], dart)

        def finish():
            ea[d] = ends
            for q in range(3):
                eu_ref[d, q] = unit[q]

        return finish

    for c in range(0, len(ranked), LOAD):
        group = range(c, min(c + LOAD, len(ranked)))
        for finish in [load(d) for d in group]:
            finish()
        for finish in [load_ends(d) for d in group]:
            finish()

    def chunks(count, body, x, ep):
        steps = -(-count // CHUNK)
        size = -(-count // steps)

        def ends(i):
            got = ends_of(lambda r: x[i, r : r + 1, :], e_ref[i])

            def finish():
                ep[i] = got

            return finish

        def step(c, carry):
            for part in (body, ends):
                for finish in [part(c * size + k) for k in range(size)]:
                    finish()
            return carry

        if steps == 1:
            step(0, 0)
        else:
            lax.fori_loop(0, steps, step, 0)

    def table_of(i, own, ghost):
        rows = {r: functools.partial(own, i, r) for r in range(SUB)}
        for a in range(3):
            down, up = near[6 * i + 2 * a], near[6 * i + 2 * a + 1]

            def into(a=a, down=down, up=up):
                return jnp.where(lower, wide(ghost(up, 4 + a)), wide(ghost(down, 4 + a)))

            def away(a=a, down=down, up=up):
                return jnp.where(lower, wide(ghost(down, a)), wide(ghost(up, a)))

            rows[SUB + a] = into
            rows[SUB + 4 + a] = away
        return rows

    def pick_ends(i, tables):
        loaded = [{number: wide(make()) for number, make in table.items()} for table in tables]
        results = []
        for end in range(2):
            row, lane = place(p_ref[i, end])
            seen = [number for number in loaded[0] if end == 1 or number < SUB + 4]
            hits = {number: row == number for number in seen}
            got = []
            for data in loaded:
                total = jnp.zeros((SUB, LANES), jnp.float32)
                for number in seen:
                    value = jnp.take_along_axis(data[number], lane, axis=1, mode="promise_in_bounds")
                    total = jnp.where(hits[number], value, total)
                got.append(total)
            results.append(got)
        return results

    def pick_two(i, own, ghost):
        one, two = pick_ends(i, [table_of(i, own, ghost)])
        return one[0], two[0]

    def couple(i):
        u = [u_ref[i, q] for q in range(3)]
        mf, mg = mf_ref[i], mg_ref[i]
        signs = [mf * jnp.where((p_ref[i, 0] & 1) == 1, -1.0, 1.0), -mg * jnp.where((p_ref[i, 1] & 1) == 1, -1.0, 1.0)]
        tables = [
            table_of(i, lambda i, r, q=q: u_ref[i, q, r : r + 1, :], lambda i, r, q=q: eu_ref[i, q, r : r + 1, :])
            for q in range(3)
        ]
        tables.append(table_of(i, lambda i, r: xa[i, r : r + 1, :], lambda i, r: ea[i, r : r + 1, :]))
        value = diag_ref[i] * xa[i]
        pulls, weights = [], []
        for end, got in enumerate(pick_ends(i, tables)):
            pull = [signs[end] * got[q] for q in range(3)]
            weight = u[0] * pull[0] + u[1] * pull[1] + u[2] * pull[2]
            value = value - weight * got[3]
            pulls = pulls + pull
            weights.append(weight)
        added = one_ref[i] + value

        def finish():
            for at, pull in enumerate(pulls):
                g_ref[i, at] = pull
            for end in range(2):
                w_ref[i, end] = weights[end]
            xb[i] = value
            one_ref[i] = added

        return finish

    chunks(counts[REACH - 1], couple, xb, eb)

    def ghost_of(ep):
        return lambda i, r: ep[i, r : r + 1, :]

    def own_of(x):
        return lambda i, r: x[i, r : r + 1, :]

    def expand(state, total, reach, first, closing):
        for term in range(first, ORDER):
            (current, ep), (following, ep_next) = state
            last = term == ORDER - 1

            def body(i, current=current, ep=ep, following=following, ep_next=ep_next, last=last):
                got = pick_two(i, own_of(current), ghost_of(ep))
                value = diag_ref[i] * current[i] - w_ref[i, 0] * got[0] - w_ref[i, 1] * got[1]
                added = total[i] + value
                if last:
                    value = closing(i, added)

                def finish():
                    total[i] = added
                    following[i] = value

                return finish

            chunks(counts[reach - term - 1], body, following, ep_next)
            state = state[::-1]
        return state

    state = expand(((xb, eb), (xa, ea)), one_ref, REACH, 1, lambda i, added: added)

    def correct(i):
        (current, ep), _ = state
        got = pick_two(i, own_of(current), ghost_of(ep))
        both = mf_ref[i] + mg_ref[i]
        scaling = lax.rsqrt(both)
        mine = both * current[i]
        length = jnp.zeros((SUB, LANES), jnp.float32)
        for q in range(3):
            part = n_ref[i, q] - scaling * (u_ref[i, q] * mine + g_ref[i, q] * got[0] + g_ref[i, 3 + q] * got[1])
            length = length + part * part
        rho = rho_ref[i]
        square = rho * rho
        value = rho - jnp.sqrt(jnp.maximum(2.0 * square - length, 0.25 * square))

        def finish():
            state[1][0][i] = value
            two_ref[i] = value

        return finish

    chunks(counts[ORDER + 1], correct, *state[1])
    state = expand(state[::-1], two_ref, ORDER + 1, 0, lambda i, added: one_ref[i] + added)
    (joint, ep_ref), (spare, _) = state

    multiplier = joint[0]
    out_mult[...] = multiplier
    for q in range(3):
        spare[q] = u_ref[0, q] * multiplier
    narrow = lower[0:1]
    total = [jnp.zeros((SUB, LANES), jnp.float32)] * 3
    for end in range(2):
        dart = own[end * SUB : (end + 1) * SUB, :]
        row, lane = place(dart)
        sign = jnp.where((dart & 1) == 1, -1.0, 1.0)
        for q in range(3):
            rows = {r: functools.partial(lambda q, r: spare[q, r : r + 1, :], q, r) for r in range(SUB)}
            total[q] = total[q] + sign * pick(rows, row, lane)
    ghost = own[2 * SUB : 3 * SUB, :]
    for q in range(3):
        rows = {}
        for a in range(3):

            def make(a=a, q=q):
                down, up = near_list[2 * a], near_list[2 * a + 1]
                at = 4 + a
                from_up = eu_ref[up, q, at : at + 1, :] * ep_ref[up, at : at + 1, :]
                from_down = eu_ref[down, q, at : at + 1, :] * ep_ref[down, at : at + 1, :]
                return jnp.where(narrow, from_up, from_down)

            rows[SUB + a] = make
        value = -mass[...] * (total[q] + pick(rows, ghost >> 7, ghost & (LANES - 1)))
        for r in range(SUB):
            out_disp[q : q + 1, r * LANES : (r + 1) * LANES] = value[r : r + 1]


def domains_near(sizes):
    def far(d, n):
        return min(d, n - d)

    ranked = sorted(
        itertools.product(*(range(n) for n in sizes)), key=lambda r: (sum(far(d, n) for d, n in zip(r, sizes)), r)
    )
    span = [sum(far(d, n) for d, n in zip(r, sizes)) for r in ranked]
    ranked = [r for r, s in zip(ranked, span) if s <= REACH]
    counts = [sum(s <= d for s in span) for d in range(REACH + 1)]
    at = {r: i for i, r in enumerate(ranked)}
    near = []
    for r in ranked:
        for a in range(3):
            for move in (-1, 1):
                to = list(r)
                to[a] = (to[a] + move) % sizes[a]
                near.append(at.get(tuple(to), 0))
    return ranked, counts, near


def per_device(old_pos, new_pos, inv_mass, rest_length, bond_pairs, live, send_index):
    sizes = [lax.axis_size(axis) for axis in AXES]
    nx, ny, nz = sizes
    atoms = old_pos.shape[1]
    width = send_index.shape[1]
    tile = (SUB, LANES)
    mass, rest, alive = (v.reshape(tile) for v in (inv_mass, rest_length, live))
    f32, i32 = jnp.float32, jnp.int32
    shape = jax.ShapeDtypeStruct

    pub, own = pl.pallas_call(
        functools.partial(publish_kernel, width),
        out_shape=[shape((FIELDS * SUB + 24, LANES), f32), shape((3 * SUB, LANES), i32)],
        in_specs=[VMEM] * 8,
        out_specs=[VMEM] * 2,
        scratch_shapes=[pltpu.VMEM(tile, i32)] * 3 + [pltpu.VMEM(tile, f32), pltpu.VMEM((2, atoms), i32)],
        name="publish",
    )(old_pos, new_pos, mass, rest, alive, live.reshape(1, atoms), bond_pairs, send_index)

    plane = ny * nz
    gathered = lax.all_to_all(jnp.broadcast_to(pub, (plane,) + pub.shape), ("gy", "gz"), 0, 0)
    parts = [gathered]
    for d in range(1, nx):
        parts.append(lax.ppermute(gathered, "gx", [(i, (i - d) % nx) for i in range(nx)]))

    ranked, counts, near = domains_near(sizes)
    held = len(ranked) + CHUNK
    near = near + [0] * (6 * (held - len(ranked)))

    def keep(*lead, kind=f32):
        return pltpu.VMEM(lead + tile, kind)

    disp, mult = pl.pallas_call(
        functools.partial(main_kernel, sizes, width, ranked, counts, near),
        out_shape=[shape((3, atoms), f32), shape(tile, f32)],
        in_specs=[VMEM] * (2 + nx),
        out_specs=[VMEM] * 2,
        scratch_shapes=[
            keep(held, 3), keep(held, 3), keep(held), keep(held), keep(held), keep(held, 2, kind=i32), keep(held, kind=i32),
            keep(held, 3), keep(held, 6), keep(held, 2), keep(held), keep(held), keep(held), keep(held), keep(held), keep(held), keep(held),
            pltpu.SMEM((len(near),), i32),
        ],
        name="solve",
    )(mass, own, *parts)
    return disp, mult.reshape(atoms)


def solution(mesh):
    flat = P(AXES)
    rows = P(None, AXES)
    return jax.shard_map(
        per_device,
        mesh=mesh,
        in_specs=(rows, rows, flat, flat, rows, flat, P(AXES, None)),
        out_specs=(rows, flat),
        check_vma=False,
    )
```

```python
import functools
import itertools

import jax
import jax.numpy as jnp
import numpy as np
from jax import lax
from jax.experimental import pallas as pl
from jax.experimental.pallas import tpu as pltpu
from jax.sharding import PartitionSpec as P

ORDER = 4
AXES = ("gx", "gy", "gz")
LANES = 128
HALF = LANES // 2
SUB = 8
CHUNK = 16
LOAD = 4
FIELDS = 11
REACH = 2 * (ORDER + 1)
VMEM = pl.BlockSpec(memory_space=pltpu.VMEM)


def wide(row):
    return jnp.broadcast_to(row, (SUB, LANES))


def pick(tables, row, lane):
    total = jnp.zeros((SUB, LANES), jnp.float32)
    for number, load in tables.items():
        got = jnp.take_along_axis(wide(load()), lane, axis=1, mode="promise_in_bounds")
        total = jnp.where(row == number, got.astype(jnp.float32), total)
    return total


def flat_rows(ref, q):
    return {r: functools.partial(lambda q, r: ref[q : q + 1, r * LANES : (r + 1) * LANES], q, r) for r in range(SUB)}


def tile_rows(ref, base=0):
    return {r: functools.partial(lambda r: ref[base + r : base + r + 1, :], r) for r in range(SUB)}


def stack_rows(ref, q, hold):
    for r in range(SUB):
        hold[r : r + 1, :] = ref[q : q + 1, r * LANES : (r + 1) * LANES]
    return hold[...]


def second_place(second, width):
    atoms = SUB * LANES
    slot = second - atoms
    block = jnp.zeros_like(second)
    for b in range(1, 6):
        block = block + (slot >= b * width).astype(jnp.int32)
    lane = slot - block * width + (block & 1) * HALF
    remote = second >= atoms
    row = jnp.where(remote, 12 + (block >> 1), second >> 7)
    return row, jnp.where(remote, lane, second & (LANES - 1))


def nt_dot(a, b):
    return lax.dot_general(a, b, (((1,), (1,)), ((), ())), preferred_element_type=jnp.float32)


def split_codes(hit, code):
    code = jnp.broadcast_to(code, hit.shape)
    zero = jnp.zeros_like(code)
    both = jnp.concatenate([jnp.where(hit, code >> 4, zero), jnp.where(hit, code & 15, zero)], 0)
    return both.astype(jnp.float32).astype(jnp.bfloat16)


def lane_hits(lane, count):
    hits = lax.broadcasted_iota(jnp.int32, (LANES, count), 0) == jnp.broadcast_to(lane, (LANES, count))
    return jnp.where(hits, 1.0, 0.0).astype(jnp.bfloat16)


def publish_kernel(width, *refs):
    far, (copies, own, mass_out), near, sems, rest_refs = refs[:8], refs[8:11], refs[11:19], refs[19], refs[20:]
    moves = [pltpu.make_async_copy(a, b, sems.at[i]) for i, (a, b) in enumerate(zip(far, near))]
    for move in moves:
        move.start()
    for move in moves:
        move.wait()
    mass_out[...] = near[2][...]
    publish_body(width, *near, copies, own, *rest_refs)


def publish_body(width, old, new, mass, rest, live, live_row, bonds, send, copies, own, pub, pad, hold_a, hold_b, s_ref, row_ref):
    atoms = SUB * LANES
    sublane = lax.broadcasted_iota(jnp.int32, (SUB, LANES), 0)
    spot = lax.broadcasted_iota(jnp.int32, (SUB, LANES), 1)
    lanes = spot[0:1]

    pad[...] = jnp.zeros_like(pad)
    pad[0:6, 0:width] = send[...]
    low = pad[...]
    high = pltpu.roll(low, HALF, 1)
    ones = [low[2 * a : 2 * a + 1] + high[2 * a + 1 : 2 * a + 2] for a in range(3)]
    for a in range(3):
        pad[a : a + 1, :] = ones[a]
    index = pad[...]
    index = jnp.where(sublane < 3, index, 0)
    sent_place = (index >> 7, index & (LANES - 1))

    first_row = bonds[0:1, :]
    second_row = bonds[1:2, :]
    usable = (live_row[...] != 0) & (first_row != second_row)
    node = lax.broadcasted_iota(jnp.int32, (1, atoms), 1)
    targets = lax.broadcasted_iota(jnp.int32, (2 * SUB, atoms), 0)
    total = jnp.zeros((4 * SUB, LANES), jnp.float32)
    places = ((first_row >> 7, first_row & (LANES - 1)), second_place(second_row, width))
    marks = []
    for end, (row, lane) in enumerate(places):
        row = jnp.where(usable, row, -1)
        hits = lane_hits(lane, atoms)
        marks.append((row, hits))
        hit = targets == jnp.broadcast_to(row, targets.shape)
        total = total + nt_dot(split_codes(hit, 2 * node + end + 1), hits)
    sums = 16.0 * total[: 2 * SUB] + total[2 * SUB :]

    valid = (lanes & (HALF - 1)) < width
    slots = jnp.zeros((2 * SUB, LANES), jnp.float32)
    for a in range(3):
        row = jnp.where(valid, ones[a] >> 7, -1)
        hit = sublane == jnp.broadcast_to(row, sublane.shape)
        slots = slots + nt_dot(split_codes(hit, (SUB + a) * LANES + lanes + 1), lane_hits(ones[a] & (LANES - 1), LANES))
    sent_slot = 16.0 * slots[:SUB] + slots[SUB:]
    s_ref[0:SUB, :] = 4096.0 * sums[:SUB] + sent_slot
    out_code = sums[SUB:]

    first = stack_rows(bonds, 0, hold_a)
    second = stack_rows(bonds, 1, hold_b)
    alive = (live[...] != 0) & (first != second)
    me = sublane * LANES + spot
    none = 2 * (2 * atoms - 1)
    table = tile_rows(s_ref)
    ends = ((first >> 7, first & (LANES - 1)), second_place(second, width))
    base = 9 * SUB
    for end, (row, lane) in enumerate(ends):
        both = pick(table, row, lane).astype(jnp.int32)
        code = (both >> 12) - (2 * me + end + 1)
        ghost = both & 4095
        link = jnp.where(code > 0, code - 1, jnp.where(ghost > 0, 2 * (ghost - 1), none))
        if end == 1:
            link = jnp.where(row >= SUB, 2 * (row * LANES + lane), link)
        pub[base + end * SUB : base + (end + 1) * SUB, :] = jnp.where(alive, link, none).astype(jnp.float32)
        lead = jnp.where(alive & (2 * me + end + 1 > code), 1, 0)
        for r in range(SUB):
            row_ref[end : end + 1, r * LANES : (r + 1) * LANES] = lead[r : r + 1]
    sent = pick(table, *sent_place).astype(jnp.int32) >> 12
    in_row = (sublane < 3) & ((spot & (HALF - 1)) < width)
    darts = jnp.where(in_row, sent - 1, jnp.where(sublane >= 4, out_code.astype(jnp.int32) - 1, -1))
    tail = FIELDS * SUB
    darts = darts.astype(jnp.float32)
    pub[tail : tail + 3, :] = darts[0:3]
    pub[tail + 3 : tail + 6, :] = darts[4:7]

    total = jnp.zeros((2 * SUB, LANES), jnp.float32)
    for end, (row, hits) in enumerate(marks):
        row = jnp.where(row_ref[end : end + 1, :] != 0, row, -1)
        hit = targets[:SUB] == jnp.broadcast_to(row, (SUB, atoms))
        total = total + nt_dot(split_codes(hit, 2 * node + end + 1), hits)
    lead = 16.0 * total[:SUB] + total[SUB:]
    own[0:SUB, :] = lead.astype(jnp.int32) - 1
    own[SUB : 2 * SUB, :] = (sums[:SUB] - lead).astype(jnp.int32) - 1
    own[2 * SUB : 3 * SUB, :] = sent_slot.astype(jnp.int32) - 1

    tables = [flat_rows(old, q) for q in range(3)] + [flat_rows(new, q) for q in range(3)] + [tile_rows(mass)]
    firsts = [pick(table, *ends[0]) for table in tables]
    seconds = [pick(table, *ends[1]) for table in tables]
    heavy = pick(tables[6], *sent_place)
    for f in range(6):
        moved = pltpu.roll(heavy, (width - f * (HALF - width)) % LANES, 1)
        got = jnp.where((spot & (HALF - 1)) < width, pick(tables[f], *sent_place), moved)
        pub[tail + 6 + 3 * f : tail + 9 + 3 * f, :] = got[0:3]
    weight = live[...].astype(jnp.float32)
    away = ends[1][0] >= SUB
    span = [weight * (x - y) for x, y in zip(firsts, seconds)]
    scaling = jnp.where(away, 1.0, lax.rsqrt(firsts[6] + seconds[6]))
    norm = jnp.where(away, 1.0, lax.rsqrt(span[0] * span[0] + span[1] * span[1] + span[2] * span[2] + 0.25))
    values = [scaling * norm * span[q] for q in range(3)]
    values = values + [scaling * span[3 + q] for q in range(3)]
    values = values + [scaling * weight * rest[...], firsts[6], seconds[6]]
    for f, value in enumerate(values):
        pub[f * SUB : (f + 1) * SUB, :] = value
    block = pub[...]

    def copy(i, carry):
        copies[i] = block
        return carry

    lax.fori_loop(0, copies.shape[0], copy, 0)


def place(dart):
    return dart >> 8, (dart >> 1) & (LANES - 1)


def main_kernel(sizes, width, ranked, counts, near_list, mass, own, *refs):
    nx, ny, nz = sizes
    pubs = refs[:nx]
    (
        out_disp, out_mult, u_ref, n_ref, rho_ref, mf_ref, mg_ref, p_ref, e_ref,
        eu_ref, g_ref, w_ref, diag_ref, xa, xb, one_ref, two_ref, ea, eb, near,
    ) = refs[nx:]
    here = (lax.axis_index("gy"), lax.axis_index("gz"))
    for at, value in enumerate(near_list):
        near[at] = value
    lower = lax.broadcasted_iota(jnp.int32, (SUB, LANES), 1) < HALF

    def wrap(value, n):
        value = jnp.where(value >= n, value - n, value)
        return jnp.where(value < 0, value + n, value)

    def source(relative):
        dx, dy, dz = (d % n for d, n in zip(relative, sizes))
        return pubs[dx], wrap(here[0] + dy, ny) * nz + wrap(here[1] + dz, nz)

    def ends_of(value, dart):
        row, lane = place(dart)
        return pick({r: functools.partial(lambda r: value(r), r) for r in range(SUB)}, row, lane)

    def load(d):
        pub, s = source(ranked[d])
        field = [pub[s, f * SUB : (f + 1) * SUB, :] for f in range(FIELDS)]
        row, lane = place(field[10].astype(jnp.int32))
        away = (row >= 12) & (row < 15)
        beside = []
        for a in range(3):
            for move in (-1, 1):
                to = list(ranked[d])
                to[a] += move
                beside.append(source(to))
        def sent_row(f, a):
            at = FIELDS * SUB + 6 + 3 * f + a
            (down, i), (up, j) = beside[2 * a], beside[2 * a + 1]
            return jnp.where(lower, wide(down[i, at : at + 1, :]), wide(up[j, at : at + 1, :]))

        sent = {(f, a): sent_row(f, a) for f in range(6) for a in range(3)}
        remote = [pick({12 + a: functools.partial(sent.get, (f, a)) for a in range(3)}, row, lane) for f in range(6)]
        spare = HALF - width
        inner = lane & (HALF - 1)
        piece = sum((inner >= f * spare).astype(jnp.int32) for f in range(1, -(-width // spare)))
        tables = {16 * f + 12 + a: functools.partial(sent.get, (f, a)) for f in range(-(-width // spare)) for a in range(3)}
        remote.append(pick(tables, 16 * piece + row, (lane - inner) + width + inner - piece * spare))
        span = [field[q] - remote[q] for q in range(6)]
        mf = field[7]
        mg = jnp.where(away, remote[6], field[8])
        both = mf + mg
        scaling = lax.rsqrt(both)
        norm = scaling * lax.rsqrt(span[0] * span[0] + span[1] * span[1] + span[2] * span[2] + 0.25)
        u = [jnp.where(away, norm * span[q], field[q]) for q in range(3)]
        n = [jnp.where(away, scaling * span[3 + q], field[3 + q]) for q in range(3)]
        rho = jnp.where(away, scaling * field[6], field[6])
        root = both * scaling
        size = u[0] * u[0] + u[1] * u[1] + u[2] * u[2]
        dot = u[0] * n[0] + u[1] * n[1] + u[2] * n[2]
        value = dot * root - rho
        at = FIELDS * SUB
        darts = [pub[s, at + 3 * h : at + 3 * h + 3, :].astype(jnp.int32) for h in range(2)]

        def finish():
            diag_ref[d] = 1.0 - both * size
            xa[d] = value
            one_ref[d] = value
            for q in range(3):
                u_ref[d, q] = u[q]
                n_ref[d, q] = n[q]
            rho_ref[d] = rho
            mf_ref[d] = mf
            mg_ref[d] = mg
            p_ref[d, 0] = field[9].astype(jnp.int32)
            p_ref[d, 1] = field[10].astype(jnp.int32)
            e_ref[d] = jnp.full((SUB, LANES), -1, jnp.int32)
            e_ref[d, 0:3] = darts[0]
            e_ref[d, 4:7] = darts[1]

        return finish

    def load_ends(d):
        dart = e_ref[d]
        sign = jnp.where((dart & 1) == 1, -1.0, 1.0)
        unit = [sign * ends_of(lambda r, q=q: u_ref[d, q, r : r + 1, :], dart) for q in range(3)]
        ends = ends_of(lambda r: xa[d, r : r + 1, :], dart)

        def finish():
            ea[d] = ends
            for q in range(3):
                eu_ref[d, q] = unit[q]

        return finish

    for c in range(0, len(ranked), LOAD):
        group = range(c, min(c + LOAD, len(ranked)))
        for finish in [load(d) for d in group]:
            finish()
        for finish in [load_ends(d) for d in group]:
            finish()

    def chunks(count, body, x, ep):
        steps = -(-count // CHUNK)
        size = -(-count // steps)

        def ends(i):
            got = ends_of(lambda r: x[i, r : r + 1, :], e_ref[i])

            def finish():
                ep[i] = got

            return finish

        def step(c, carry):
            for part in (body, ends):
                for finish in [part(c * size + k) for k in range(size)]:
                    finish()
            return carry

        if steps == 1:
            step(0, 0)
        else:
            lax.fori_loop(0, steps, step, 0)

    def table_of(i, own, ghost):
        rows = {r: functools.partial(own, i, r) for r in range(SUB)}
        for a in range(3):
            down, up = near[6 * i + 2 * a], near[6 * i + 2 * a + 1]

            def into(a=a, down=down, up=up):
                return jnp.where(lower, wide(ghost(up, 4 + a)), wide(ghost(down, 4 + a)))

            def away(a=a, down=down, up=up):
                return jnp.where(lower, wide(ghost(down, a)), wide(ghost(up, a)))

            rows[SUB + a] = into
            rows[SUB + 4 + a] = away
        return rows

    def pick_ends(i, tables):
        loaded = [{number: wide(make()) for number, make in table.items()} for table in tables]
        results = []
        for end in range(2):
            row, lane = place(p_ref[i, end])
            seen = [number for number in loaded[0] if end == 1 or number < SUB + 4]
            hits = {number: row == number for number in seen}
            got = []
            for data in loaded:
                total = jnp.zeros((SUB, LANES), jnp.float32)
                for number in seen:
                    value = jnp.take_along_axis(data[number], lane, axis=1, mode="promise_in_bounds")
                    total = jnp.where(hits[number], value, total)
                got.append(total)
            results.append(got)
        return results

    def pick_two(i, own, ghost):
        one, two = pick_ends(i, [table_of(i, own, ghost)])
        return one[0], two[0]

    def couple(i):
        u = [u_ref[i, q] for q in range(3)]
        mf, mg = mf_ref[i], mg_ref[i]
        signs = [mf * jnp.where((p_ref[i, 0] & 1) == 1, -1.0, 1.0), -mg * jnp.where((p_ref[i, 1] & 1) == 1, -1.0, 1.0)]
        tables = [
            table_of(i, lambda i, r, q=q: u_ref[i, q, r : r + 1, :], lambda i, r, q=q: eu_ref[i, q, r : r + 1, :])
            for q in range(3)
        ]
        tables.append(table_of(i, lambda i, r: xa[i, r : r + 1, :], lambda i, r: ea[i, r : r + 1, :]))
        value = diag_ref[i] * xa[i]
        pulls, weights = [], []
        for end, got in enumerate(pick_ends(i, tables)):
            pull = [signs[end] * got[q] for q in range(3)]
            weight = u[0] * pull[0] + u[1] * pull[1] + u[2] * pull[2]
            value = value - weight * got[3]
            pulls = pulls + pull
            weights.append(weight)
        added = one_ref[i] + value

        def finish():
            for at, pull in enumerate(pulls):
                g_ref[i, at] = pull
            for end in range(2):
                w_ref[i, end] = weights[end]
            xb[i] = value
            one_ref[i] = added

        return finish

    chunks(counts[REACH - 1], couple, xb, eb)

    def ghost_of(ep):
        return lambda i, r: ep[i, r : r + 1, :]

    def own_of(x):
        return lambda i, r: x[i, r : r + 1, :]

    def expand(state, total, reach, first, closing):
        for term in range(first, ORDER):
            (current, ep), (following, ep_next) = state
            last = term == ORDER - 1

            def body(i, current=current, ep=ep, following=following, ep_next=ep_next, last=last):
                got = pick_two(i, own_of(current), ghost_of(ep))
                value = diag_ref[i] * current[i] - w_ref[i, 0] * got[0] - w_ref[i, 1] * got[1]
                added = total[i] + value
                if last:
                    value = closing(i, added)

                def finish():
                    total[i] = added
                    following[i] = value

                return finish

            chunks(counts[reach - term - 1], body, following, ep_next)
            state = state[::-1]
        return state

    state = expand(((xb, eb), (xa, ea)), one_ref, REACH, 1, lambda i, added: added)

    def correct(i):
        (current, ep), _ = state
        got = pick_two(i, own_of(current), ghost_of(ep))
        both = mf_ref[i] + mg_ref[i]
        scaling = lax.rsqrt(both)
        mine = both * current[i]
        length = jnp.zeros((SUB, LANES), jnp.float32)
        for q in range(3):
            part = n_ref[i, q] - scaling * (u_ref[i, q] * mine + g_ref[i, q] * got[0] + g_ref[i, 3 + q] * got[1])
            length = length + part * part
        rho = rho_ref[i]
        square = rho * rho
        value = rho - jnp.sqrt(jnp.maximum(2.0 * square - length, 0.25 * square))

        def finish():
            state[1][0][i] = value
            two_ref[i] = value

        return finish

    chunks(counts[ORDER + 1], correct, *state[1])
    state = expand(state[::-1], two_ref, ORDER + 1, 0, lambda i, added: one_ref[i] + added)
    (joint, ep_ref), (spare, _) = state

    multiplier = joint[0]
    out_mult[...] = multiplier
    for q in range(3):
        spare[q] = u_ref[0, q] * multiplier
    narrow = lower[0:1]
    total = [jnp.zeros((SUB, LANES), jnp.float32)] * 3
    for end in range(2):
        dart = own[end * SUB : (end + 1) * SUB, :]
        row, lane = place(dart)
        sign = jnp.where((dart & 1) == 1, -1.0, 1.0)
        for q in range(3):
            rows = {r: functools.partial(lambda q, r: spare[q, r : r + 1, :], q, r) for r in range(SUB)}
            total[q] = total[q] + sign * pick(rows, row, lane)
    ghost = own[2 * SUB : 3 * SUB, :]
    for q in range(3):
        rows = {}
        for a in range(3):

            def make(a=a, q=q):
                down, up = near_list[2 * a], near_list[2 * a + 1]
                at = 4 + a
                from_up = eu_ref[up, q, at : at + 1, :] * ep_ref[up, at : at + 1, :]
                from_down = eu_ref[down, q, at : at + 1, :] * ep_ref[down, at : at + 1, :]
                return jnp.where(narrow, from_up, from_down)

            rows[SUB + a] = make
        value = -mass[...] * (total[q] + pick(rows, ghost >> 7, ghost & (LANES - 1)))
        for r in range(SUB):
            out_disp[q : q + 1, r * LANES : (r + 1) * LANES] = value[r : r + 1]


def domains_near(sizes):
    def far(d, n):
        return min(d, n - d)

    ranked = sorted(
        itertools.product(*(range(n) for n in sizes)), key=lambda r: (sum(far(d, n) for d, n in zip(r, sizes)), r)
    )
    span = [sum(far(d, n) for d, n in zip(r, sizes)) for r in ranked]
    ranked = [r for r, s in zip(ranked, span) if s <= REACH]
    counts = [sum(s <= d for s in span) for d in range(REACH + 1)]
    at = {r: i for i, r in enumerate(ranked)}
    near = []
    for r in ranked:
        for a in range(3):
            for move in (-1, 1):
                to = list(r)
                to[a] = (to[a] + move) % sizes[a]
                near.append(at.get(tuple(to), 0))
    return ranked, counts, near


def per_device(old_pos, new_pos, inv_mass, rest_length, bond_pairs, live, send_index):
    sizes = [lax.axis_size(axis) for axis in AXES]
    nx, ny, nz = sizes
    atoms = old_pos.shape[1]
    width = send_index.shape[1]
    tile = (SUB, LANES)
    mass, rest, alive = (v.reshape(tile) for v in (inv_mass, rest_length, live))
    f32, i32 = jnp.float32, jnp.int32
    shape = jax.ShapeDtypeStruct

    inputs = (old_pos, new_pos, mass, rest, alive, live.reshape(1, atoms), bond_pairs, send_index)
    block = (FIELDS * SUB + 24, LANES)
    pub, own, mass = pl.pallas_call(
        functools.partial(publish_kernel, width),
        out_shape=[shape((ny * nz,) + block, f32), shape((3 * SUB, LANES), i32), shape(tile, f32)],
        in_specs=[pl.BlockSpec(memory_space=pltpu.MemorySpace.HBM)] * len(inputs),
        out_specs=[VMEM] * 3,
        scratch_shapes=[pltpu.VMEM(v.shape, v.dtype) for v in inputs]
        + [pltpu.SemaphoreType.DMA((len(inputs),)), pltpu.VMEM(block, f32)]
        + [pltpu.VMEM(tile, i32)] * 3
        + [pltpu.VMEM(tile, f32), pltpu.VMEM((2, atoms), i32)],
        name="publish",
    )(*inputs)

    gathered = lax.all_to_all(pub, ("gy", "gz"), 0, 0)
    parts = [gathered]
    for d in range(1, nx):
        parts.append(lax.ppermute(gathered, "gx", [(i, (i - d) % nx) for i in range(nx)]))

    ranked, counts, near = domains_near(sizes)
    held = len(ranked) + CHUNK
    near = near + [0] * (6 * (held - len(ranked)))

    def keep(*lead, kind=f32):
        return pltpu.VMEM(lead + tile, kind)

    disp, mult = pl.pallas_call(
        functools.partial(main_kernel, sizes, width, ranked, counts, near),
        out_shape=[shape((3, atoms), f32), shape(tile, f32)],
        in_specs=[VMEM] * (2 + nx),
        out_specs=[VMEM] * 2,
        scratch_shapes=[
            keep(held, 3), keep(held, 3), keep(held), keep(held), keep(held), keep(held, 2, kind=i32), keep(held, kind=i32),
            keep(held, 3), keep(held, 6), keep(held, 2), keep(held), keep(held), keep(held), keep(held), keep(held), keep(held), keep(held),
            pltpu.SMEM((len(near),), i32),
        ],
        compiler_params=pltpu.CompilerParams(vmem_limit_bytes=24 << 20),
        name="solve",
    )(mass, own, *parts)
    return disp, mult.reshape(atoms)


def solution(mesh):
    flat = P(AXES)
    rows = P(None, AXES)
    return jax.shard_map(
        per_device,
        mesh=mesh,
        in_specs=(rows, rows, flat, flat, rows, flat, P(AXES, None)),
        out_specs=(rows, flat),
        check_vma=False,
    )
```

```python
import functools
import itertools

import jax
import jax.numpy as jnp
import numpy as np
from jax import lax
from jax.experimental import pallas as pl
from jax.experimental.pallas import tpu as pltpu
from jax.sharding import PartitionSpec as P

ORDER = 4
AXES = ("gx", "gy", "gz")
LANES = 128
HALF = LANES // 2
SUB = 8
CHUNK = 32
LOAD = 8
FIELDS = 11
REACH = 2 * (ORDER + 1)
VMEM = pl.BlockSpec(memory_space=pltpu.VMEM)


def wide(row):
    return jnp.broadcast_to(row, (SUB, LANES))


def pick(tables, row, lane):
    total = jnp.zeros((SUB, LANES), jnp.float32)
    for number, load in tables.items():
        got = jnp.take_along_axis(wide(load()), lane, axis=1, mode="promise_in_bounds")
        total = jnp.where(row == number, got.astype(jnp.float32), total)
    return total


def flat_rows(ref, q):
    return {r: functools.partial(lambda q, r: ref[q : q + 1, r * LANES : (r + 1) * LANES], q, r) for r in range(SUB)}


def tile_rows(ref, base=0):
    return {r: functools.partial(lambda r: ref[base + r : base + r + 1, :], r) for r in range(SUB)}


def stack_rows(ref, q, hold):
    for r in range(SUB):
        hold[r : r + 1, :] = ref[q : q + 1, r * LANES : (r + 1) * LANES]
    return hold[...]


def second_place(second, width):
    atoms = SUB * LANES
    slot = second - atoms
    block = jnp.zeros_like(second)
    for b in range(1, 6):
        block = block + (slot >= b * width).astype(jnp.int32)
    lane = slot - block * width + (block & 1) * HALF
    remote = second >= atoms
    row = jnp.where(remote, 12 + (block >> 1), second >> 7)
    return row, jnp.where(remote, lane, second & (LANES - 1))


def nt_dot(a, b):
    return lax.dot_general(a, b, (((1,), (1,)), ((), ())), preferred_element_type=jnp.float32)


def split_codes(hit, code):
    code = jnp.broadcast_to(code, hit.shape)
    zero = jnp.zeros_like(code)
    both = jnp.concatenate([jnp.where(hit, code >> 4, zero), jnp.where(hit, code & 15, zero)], 0)
    return both.astype(jnp.float32).astype(jnp.bfloat16)


def lane_hits(lane, count):
    hits = lax.broadcasted_iota(jnp.int32, (LANES, count), 0) == jnp.broadcast_to(lane, (LANES, count))
    return jnp.where(hits, 1.0, 0.0).astype(jnp.bfloat16)


def publish_kernel(width, *refs):
    far, (copies, own, mass_out), near, sems, rest_refs = refs[:8], refs[8:11], refs[11:19], refs[19], refs[20:]
    moves = [pltpu.make_async_copy(a, b, sems.at[i]) for i, (a, b) in enumerate(zip(far, near))]
    for move in moves:
        move.start()
    for move in moves:
        move.wait()
    mass_out[...] = near[2][...]
    publish_body(width, *near, copies, own, *rest_refs)


def publish_body(width, old, new, mass, rest, live, live_row, bonds, send, copies, own, pub, pad, hold_a, hold_b, s_ref, row_ref):
    atoms = SUB * LANES
    sublane = lax.broadcasted_iota(jnp.int32, (SUB, LANES), 0)
    spot = lax.broadcasted_iota(jnp.int32, (SUB, LANES), 1)
    lanes = spot[0:1]

    pad[...] = jnp.zeros_like(pad)
    pad[0:6, 0:width] = send[...]
    low = pad[...]
    high = pltpu.roll(low, HALF, 1)
    ones = [low[2 * a : 2 * a + 1] + high[2 * a + 1 : 2 * a + 2] for a in range(3)]
    for a in range(3):
        pad[a : a + 1, :] = ones[a]
    index = pad[...]
    index = jnp.where(sublane < 3, index, 0)
    sent_place = (index >> 7, index & (LANES - 1))

    first_row = bonds[0:1, :]
    second_row = bonds[1:2, :]
    usable = (live_row[...] != 0) & (first_row != second_row)
    node = lax.broadcasted_iota(jnp.int32, (1, atoms), 1)
    targets = lax.broadcasted_iota(jnp.int32, (2 * SUB, atoms), 0)
    total = jnp.zeros((4 * SUB, LANES), jnp.float32)
    places = ((first_row >> 7, first_row & (LANES - 1)), second_place(second_row, width))
    marks = []
    for end, (row, lane) in enumerate(places):
        row = jnp.where(usable, row, -1)
        hits = lane_hits(lane, atoms)
        marks.append((row, hits))
        hit = targets == jnp.broadcast_to(row, targets.shape)
        total = total + nt_dot(split_codes(hit, 2 * node + end + 1), hits)
    sums = 16.0 * total[: 2 * SUB] + total[2 * SUB :]

    valid = (lanes & (HALF - 1)) < width
    slots = jnp.zeros((2 * SUB, LANES), jnp.float32)
    for a in range(3):
        row = jnp.where(valid, ones[a] >> 7, -1)
        hit = sublane == jnp.broadcast_to(row, sublane.shape)
        slots = slots + nt_dot(split_codes(hit, (SUB + a) * LANES + lanes + 1), lane_hits(ones[a] & (LANES - 1), LANES))
    sent_slot = 16.0 * slots[:SUB] + slots[SUB:]
    s_ref[0:SUB, :] = 4096.0 * sums[:SUB] + sent_slot
    out_code = sums[SUB:]

    first = stack_rows(bonds, 0, hold_a)
    second = stack_rows(bonds, 1, hold_b)
    alive = (live[...] != 0) & (first != second)
    me = sublane * LANES + spot
    none = 2 * (2 * atoms - 1)
    table = tile_rows(s_ref)
    ends = ((first >> 7, first & (LANES - 1)), second_place(second, width))
    base = 9 * SUB
    for end, (row, lane) in enumerate(ends):
        both = pick(table, row, lane).astype(jnp.int32)
        code = (both >> 12) - (2 * me + end + 1)
        ghost = both & 4095
        link = jnp.where(code > 0, code - 1, jnp.where(ghost > 0, 2 * (ghost - 1), none))
        if end == 1:
            link = jnp.where(row >= SUB, 2 * (row * LANES + lane), link)
        pub[base + end * SUB : base + (end + 1) * SUB, :] = jnp.where(alive, link, none).astype(jnp.float32)
        lead = jnp.where(alive & (2 * me + end + 1 > code), 1, 0)
        for r in range(SUB):
            row_ref[end : end + 1, r * LANES : (r + 1) * LANES] = lead[r : r + 1]
    sent = pick(table, *sent_place).astype(jnp.int32) >> 12
    in_row = (sublane < 3) & ((spot & (HALF - 1)) < width)
    darts = jnp.where(in_row, sent - 1, jnp.where(sublane >= 4, out_code.astype(jnp.int32) - 1, -1))
    tail = FIELDS * SUB
    darts = darts.astype(jnp.float32)
    pub[tail : tail + 3, :] = darts[0:3]
    pub[tail + 3 : tail + 6, :] = darts[4:7]

    total = jnp.zeros((2 * SUB, LANES), jnp.float32)
    for end, (row, hits) in enumerate(marks):
        row = jnp.where(row_ref[end : end + 1, :] != 0, row, -1)
        hit = targets[:SUB] == jnp.broadcast_to(row, (SUB, atoms))
        total = total + nt_dot(split_codes(hit, 2 * node + end + 1), hits)
    lead = 16.0 * total[:SUB] + total[SUB:]
    own[0:SUB, :] = lead.astype(jnp.int32) - 1
    own[SUB : 2 * SUB, :] = (sums[:SUB] - lead).astype(jnp.int32) - 1
    own[2 * SUB : 3 * SUB, :] = sent_slot.astype(jnp.int32) - 1

    tables = [flat_rows(old, q) for q in range(3)] + [flat_rows(new, q) for q in range(3)] + [tile_rows(mass)]
    firsts = [pick(table, *ends[0]) for table in tables]
    seconds = [pick(table, *ends[1]) for table in tables]
    heavy = pick(tables[6], *sent_place)
    for f in range(6):
        moved = pltpu.roll(heavy, (width - f * (HALF - width)) % LANES, 1)
        got = jnp.where((spot & (HALF - 1)) < width, pick(tables[f], *sent_place), moved)
        pub[tail + 6 + 3 * f : tail + 9 + 3 * f, :] = got[0:3]
    weight = live[...].astype(jnp.float32)
    away = ends[1][0] >= SUB
    span = [weight * (x - y) for x, y in zip(firsts, seconds)]
    scaling = jnp.where(away, 1.0, lax.rsqrt(firsts[6] + seconds[6]))
    norm = jnp.where(away, 1.0, lax.rsqrt(span[0] * span[0] + span[1] * span[1] + span[2] * span[2] + 0.25))
    values = [scaling * norm * span[q] for q in range(3)]
    values = values + [scaling * span[3 + q] for q in range(3)]
    values = values + [scaling * weight * rest[...], firsts[6], seconds[6]]
    for f, value in enumerate(values):
        pub[f * SUB : (f + 1) * SUB, :] = value
    block = pub[...]

    def copy(i, carry):
        copies[i] = block
        return carry

    lax.fori_loop(0, copies.shape[0], copy, 0)


def place(dart):
    return dart >> 8, (dart >> 1) & (LANES - 1)


def main_kernel(sizes, width, ranked, counts, near_list, mass, own, *refs):
    nx, ny, nz = sizes
    pubs = refs[:nx]
    (
        out_disp, out_mult, u_ref, n_ref, rho_ref, mf_ref, mg_ref, p_ref, e_ref,
        eu_ref, g_ref, w_ref, diag_ref, xa, xb, one_ref, two_ref, ea, eb, near,
    ) = refs[nx:]
    here = (lax.axis_index("gy"), lax.axis_index("gz"))
    for at, value in enumerate(near_list):
        near[at] = value
    lower = lax.broadcasted_iota(jnp.int32, (SUB, LANES), 1) < HALF

    def wrap(value, n):
        value = jnp.where(value >= n, value - n, value)
        return jnp.where(value < 0, value + n, value)

    def source(relative):
        dx, dy, dz = (d % n for d, n in zip(relative, sizes))
        return pubs[dx], wrap(here[0] + dy, ny) * nz + wrap(here[1] + dz, nz)

    def ends_of(value, dart):
        row, lane = place(dart)
        return pick({r: functools.partial(lambda r: value(r), r) for r in range(SUB)}, row, lane)

    def load(d):
        pub, s = source(ranked[d])
        field = [pub[s, f * SUB : (f + 1) * SUB, :] for f in range(FIELDS)]
        row, lane = place(field[10].astype(jnp.int32))
        away = (row >= 12) & (row < 15)
        beside = []
        for a in range(3):
            for move in (-1, 1):
                to = list(ranked[d])
                to[a] += move
                beside.append(source(to))
        def sent_row(f, a):
            at = FIELDS * SUB + 6 + 3 * f + a
            (down, i), (up, j) = beside[2 * a], beside[2 * a + 1]
            return jnp.where(lower, wide(down[i, at : at + 1, :]), wide(up[j, at : at + 1, :]))

        sent = {(f, a): sent_row(f, a) for f in range(6) for a in range(3)}
        remote = [pick({12 + a: functools.partial(sent.get, (f, a)) for a in range(3)}, row, lane) for f in range(6)]
        spare = HALF - width
        inner = lane & (HALF - 1)
        piece = sum((inner >= f * spare).astype(jnp.int32) for f in range(1, -(-width // spare)))
        tables = {16 * f + 12 + a: functools.partial(sent.get, (f, a)) for f in range(-(-width // spare)) for a in range(3)}
        remote.append(pick(tables, 16 * piece + row, (lane - inner) + width + inner - piece * spare))
        span = [field[q] - remote[q] for q in range(6)]
        mf = field[7]
        mg = jnp.where(away, remote[6], field[8])
        both = mf + mg
        scaling = lax.rsqrt(both)
        norm = scaling * lax.rsqrt(span[0] * span[0] + span[1] * span[1] + span[2] * span[2] + 0.25)
        u = [jnp.where(away, norm * span[q], field[q]) for q in range(3)]
        n = [jnp.where(away, scaling * span[3 + q], field[3 + q]) for q in range(3)]
        rho = jnp.where(away, scaling * field[6], field[6])
        root = both * scaling
        size = u[0] * u[0] + u[1] * u[1] + u[2] * u[2]
        dot = u[0] * n[0] + u[1] * n[1] + u[2] * n[2]
        value = dot * root - rho
        at = FIELDS * SUB
        darts = [pub[s, at + 3 * h : at + 3 * h + 3, :].astype(jnp.int32) for h in range(2)]

        def finish():
            diag_ref[d] = 1.0 - both * size
            xa[d] = value
            one_ref[d] = value
            for q in range(3):
                u_ref[d, q] = u[q]
                n_ref[d, q] = n[q]
            rho_ref[d] = rho
            mf_ref[d] = mf
            mg_ref[d] = mg
            p_ref[d, 0] = field[9].astype(jnp.int32)
            p_ref[d, 1] = field[10].astype(jnp.int32)
            e_ref[d] = jnp.full((SUB, LANES), -1, jnp.int32)
            e_ref[d, 0:3] = darts[0]
            e_ref[d, 4:7] = darts[1]

        return finish

    def load_ends(d):
        dart = e_ref[d]
        sign = jnp.where((dart & 1) == 1, -1.0, 1.0)
        unit = [sign * ends_of(lambda r, q=q: u_ref[d, q, r : r + 1, :], dart) for q in range(3)]
        ends = ends_of(lambda r: xa[d, r : r + 1, :], dart)

        def finish():
            ea[d] = ends
            for q in range(3):
                eu_ref[d, q] = unit[q]

        return finish

    for c in range(0, len(ranked), LOAD):
        group = range(c, min(c + LOAD, len(ranked)))
        for finish in [load(d) for d in group]:
            finish()
        for finish in [load_ends(d) for d in group]:
            finish()

    def chunks(count, body, x, ep):
        steps = -(-count // CHUNK)
        size = -(-count // steps)

        def ends(i):
            got = ends_of(lambda r: x[i, r : r + 1, :], e_ref[i])

            def finish():
                ep[i] = got

            return finish

        def step(c, carry):
            for part in (body, ends):
                for finish in [part(c * size + k) for k in range(size)]:
                    finish()
            return carry

        if steps == 1:
            step(0, 0)
        else:
            lax.fori_loop(0, steps, step, 0)

    def table_of(i, own, ghost):
        rows = {r: functools.partial(own, i, r) for r in range(SUB)}
        for a in range(3):
            table = near_list if isinstance(i, int) else near
            down, up = table[6 * i + 2 * a], table[6 * i + 2 * a + 1]

            def into(a=a, down=down, up=up):
                return jnp.where(lower, wide(ghost(up, 4 + a)), wide(ghost(down, 4 + a)))

            def away(a=a, down=down, up=up):
                return jnp.where(lower, wide(ghost(down, a)), wide(ghost(up, a)))

            rows[SUB + a] = into
            rows[SUB + 4 + a] = away
        return rows

    def pick_ends(i, tables):
        loaded = [{number: wide(make()) for number, make in table.items()} for table in tables]
        results = []
        for end in range(2):
            row, lane = place(p_ref[i, end])
            seen = [number for number in loaded[0] if end == 1 or number < SUB + 4]
            hits = {number: row == number for number in seen}
            got = []
            for data in loaded:
                total = jnp.zeros((SUB, LANES), jnp.float32)
                for number in seen:
                    value = jnp.take_along_axis(data[number], lane, axis=1, mode="promise_in_bounds")
                    total = jnp.where(hits[number], value, total)
                got.append(total)
            results.append(got)
        return results

    def pick_two(i, own, ghost):
        one, two = pick_ends(i, [table_of(i, own, ghost)])
        return one[0], two[0]

    def couple(i):
        u = [u_ref[i, q] for q in range(3)]
        mf, mg = mf_ref[i], mg_ref[i]
        signs = [mf * jnp.where((p_ref[i, 0] & 1) == 1, -1.0, 1.0), -mg * jnp.where((p_ref[i, 1] & 1) == 1, -1.0, 1.0)]
        tables = [
            table_of(i, lambda i, r, q=q: u_ref[i, q, r : r + 1, :], lambda i, r, q=q: eu_ref[i, q, r : r + 1, :])
            for q in range(3)
        ]
        tables.append(table_of(i, lambda i, r: xa[i, r : r + 1, :], lambda i, r: ea[i, r : r + 1, :]))
        value = diag_ref[i] * xa[i]
        pulls, weights = [], []
        for end, got in enumerate(pick_ends(i, tables)):
            pull = [signs[end] * got[q] for q in range(3)]
            weight = u[0] * pull[0] + u[1] * pull[1] + u[2] * pull[2]
            value = value - weight * got[3]
            pulls = pulls + pull
            weights.append(weight)
        added = one_ref[i] + value

        def finish():
            for at, pull in enumerate(pulls):
                g_ref[i, at] = pull
            for end in range(2):
                w_ref[i, end] = weights[end]
            xb[i] = value
            one_ref[i] = added

        return finish

    chunks(counts[REACH - 1], couple, xb, eb)

    def ghost_of(ep):
        return lambda i, r: ep[i, r : r + 1, :]

    def own_of(x):
        return lambda i, r: x[i, r : r + 1, :]

    def expand(state, total, reach, first, closing):
        for term in range(first, ORDER):
            (current, ep), (following, ep_next) = state
            last = term == ORDER - 1

            def body(i, current=current, ep=ep, following=following, ep_next=ep_next, last=last):
                got = pick_two(i, own_of(current), ghost_of(ep))
                value = diag_ref[i] * current[i] - w_ref[i, 0] * got[0] - w_ref[i, 1] * got[1]
                added = total[i] + value
                if last:
                    value = closing(i, added)

                def finish():
                    total[i] = added
                    following[i] = value

                return finish

            chunks(counts[reach - term - 1], body, following, ep_next)
            state = state[::-1]
        return state

    state = expand(((xb, eb), (xa, ea)), one_ref, REACH, 1, lambda i, added: added)

    def correct(i):
        (current, ep), _ = state
        got = pick_two(i, own_of(current), ghost_of(ep))
        both = mf_ref[i] + mg_ref[i]
        scaling = lax.rsqrt(both)
        mine = both * current[i]
        length = jnp.zeros((SUB, LANES), jnp.float32)
        for q in range(3):
            part = n_ref[i, q] - scaling * (u_ref[i, q] * mine + g_ref[i, q] * got[0] + g_ref[i, 3 + q] * got[1])
            length = length + part * part
        rho = rho_ref[i]
        square = rho * rho
        value = rho - jnp.sqrt(jnp.maximum(2.0 * square - length, 0.25 * square))

        def finish():
            state[1][0][i] = value
            two_ref[i] = value

        return finish

    chunks(counts[ORDER + 1], correct, *state[1])
    state = expand(state[::-1], two_ref, ORDER + 1, 0, lambda i, added: one_ref[i] + added)
    (joint, ep_ref), (spare, _) = state

    multiplier = joint[0]
    out_mult[...] = multiplier
    for q in range(3):
        spare[q] = u_ref[0, q] * multiplier
    narrow = lower[0:1]
    total = [jnp.zeros((SUB, LANES), jnp.float32)] * 3
    for end in range(2):
        dart = own[end * SUB : (end + 1) * SUB, :]
        row, lane = place(dart)
        sign = jnp.where((dart & 1) == 1, -1.0, 1.0)
        for q in range(3):
            rows = {r: functools.partial(lambda q, r: spare[q, r : r + 1, :], q, r) for r in range(SUB)}
            total[q] = total[q] + sign * pick(rows, row, lane)
    ghost = own[2 * SUB : 3 * SUB, :]
    for q in range(3):
        rows = {}
        for a in range(3):

            def make(a=a, q=q):
                down, up = near_list[2 * a], near_list[2 * a + 1]
                at = 4 + a
                from_up = eu_ref[up, q, at : at + 1, :] * ep_ref[up, at : at + 1, :]
                from_down = eu_ref[down, q, at : at + 1, :] * ep_ref[down, at : at + 1, :]
                return jnp.where(narrow, from_up, from_down)

            rows[SUB + a] = make
        value = -mass[...] * (total[q] + pick(rows, ghost >> 7, ghost & (LANES - 1)))
        for r in range(SUB):
            out_disp[q : q + 1, r * LANES : (r + 1) * LANES] = value[r : r + 1]


def domains_near(sizes):
    def far(d, n):
        return min(d, n - d)

    ranked = sorted(
        itertools.product(*(range(n) for n in sizes)), key=lambda r: (sum(far(d, n) for d, n in zip(r, sizes)), r)
    )
    span = [sum(far(d, n) for d, n in zip(r, sizes)) for r in ranked]
    ranked = [r for r, s in zip(ranked, span) if s <= REACH]
    counts = [sum(s <= d for s in span) for d in range(REACH + 1)]
    at = {r: i for i, r in enumerate(ranked)}
    near = []
    for r in ranked:
        for a in range(3):
            for move in (-1, 1):
                to = list(r)
                to[a] = (to[a] + move) % sizes[a]
                near.append(at.get(tuple(to), 0))
    return ranked, counts, near


def per_device(old_pos, new_pos, inv_mass, rest_length, bond_pairs, live, send_index):
    sizes = [lax.axis_size(axis) for axis in AXES]
    nx, ny, nz = sizes
    atoms = old_pos.shape[1]
    width = send_index.shape[1]
    tile = (SUB, LANES)
    mass, rest, alive = (v.reshape(tile) for v in (inv_mass, rest_length, live))
    f32, i32 = jnp.float32, jnp.int32
    shape = jax.ShapeDtypeStruct

    inputs = (old_pos, new_pos, mass, rest, alive, live.reshape(1, atoms), bond_pairs, send_index)
    block = (FIELDS * SUB + 24, LANES)
    pub, own, mass = pl.pallas_call(
        functools.partial(publish_kernel, width),
        out_shape=[shape((ny * nz,) + block, f32), shape((3 * SUB, LANES), i32), shape(tile, f32)],
        in_specs=[pl.BlockSpec(memory_space=pltpu.MemorySpace.HBM)] * len(inputs),
        out_specs=[VMEM] * 3,
        scratch_shapes=[pltpu.VMEM(v.shape, v.dtype) for v in inputs]
        + [pltpu.SemaphoreType.DMA((len(inputs),)), pltpu.VMEM(block, f32)]
        + [pltpu.VMEM(tile, i32)] * 3
        + [pltpu.VMEM(tile, f32), pltpu.VMEM((2, atoms), i32)],
        name="publish",
    )(*inputs)

    gathered = lax.all_to_all(pub, ("gy", "gz"), 0, 0)
    parts = [gathered]
    for d in range(1, nx):
        parts.append(lax.ppermute(gathered, "gx", [(i, (i - d) % nx) for i in range(nx)]))

    ranked, counts, near = domains_near(sizes)
    held = len(ranked) + CHUNK
    near = near + [0] * (6 * (held - len(ranked)))

    def keep(*lead, kind=f32):
        return pltpu.VMEM(lead + tile, kind)

    disp, mult = pl.pallas_call(
        functools.partial(main_kernel, sizes, width, ranked, counts, near),
        out_shape=[shape((3, atoms), f32), shape(tile, f32)],
        in_specs=[VMEM] * (2 + nx),
        out_specs=[VMEM] * 2,
        scratch_shapes=[
            keep(held, 3), keep(held, 3), keep(held), keep(held), keep(held), keep(held, 2, kind=i32), keep(held, kind=i32),
            keep(held, 3), keep(held, 6), keep(held, 2), keep(held), keep(held), keep(held), keep(held), keep(held), keep(held), keep(held),
            pltpu.SMEM((len(near),), i32),
        ],
        compiler_params=pltpu.CompilerParams(vmem_limit_bytes=24 << 20),
        name="solve",
    )(mass, own, *parts)
    return disp, mult.reshape(atoms)


def solution(mesh):
    flat = P(AXES)
    rows = P(None, AXES)
    return jax.shard_map(
        per_device,
        mesh=mesh,
        in_specs=(rows, rows, flat, flat, rows, flat, P(AXES, None)),
        out_specs=(rows, flat),
        check_vma=False,
    )
```

```python
import functools
import itertools

import jax
import jax.numpy as jnp
import numpy as np
from jax import lax
from jax.experimental import pallas as pl
from jax.experimental.pallas import tpu as pltpu
from jax.sharding import PartitionSpec as P

ORDER = 4
AXES = ("gx", "gy", "gz")
LANES = 128
HALF = LANES // 2
SUB = 8
CHUNK = 32
LOAD = 16
FIELDS = 11
REACH = 2 * (ORDER + 1)
VMEM = pl.BlockSpec(memory_space=pltpu.VMEM)


def wide(row):
    return jnp.broadcast_to(row, (SUB, LANES))


def pick(tables, row, lane):
    total = jnp.zeros((SUB, LANES), jnp.float32)
    for number, load in tables.items():
        got = jnp.take_along_axis(wide(load()), lane, axis=1, mode="promise_in_bounds")
        total = jnp.where(row == number, got.astype(jnp.float32), total)
    return total


def flat_rows(ref, q):
    return {r: functools.partial(lambda q, r: ref[q : q + 1, r * LANES : (r + 1) * LANES], q, r) for r in range(SUB)}


def tile_rows(ref, base=0):
    return {r: functools.partial(lambda r: ref[base + r : base + r + 1, :], r) for r in range(SUB)}


def stack_rows(ref, q, hold):
    for r in range(SUB):
        hold[r : r + 1, :] = ref[q : q + 1, r * LANES : (r + 1) * LANES]
    return hold[...]


def second_place(second, width):
    atoms = SUB * LANES
    slot = second - atoms
    block = jnp.zeros_like(second)
    for b in range(1, 6):
        block = block + (slot >= b * width).astype(jnp.int32)
    lane = slot - block * width + (block & 1) * HALF
    remote = second >= atoms
    row = jnp.where(remote, 12 + (block >> 1), second >> 7)
    return row, jnp.where(remote, lane, second & (LANES - 1))


def nt_dot(a, b):
    return lax.dot_general(a, b, (((1,), (1,)), ((), ())), preferred_element_type=jnp.float32)


def split_codes(hit, code):
    code = jnp.broadcast_to(code, hit.shape)
    zero = jnp.zeros_like(code)
    both = jnp.concatenate([jnp.where(hit, code >> 4, zero), jnp.where(hit, code & 15, zero)], 0)
    return both.astype(jnp.float32).astype(jnp.bfloat16)


def lane_hits(lane, count):
    hits = lax.broadcasted_iota(jnp.int32, (LANES, count), 0) == jnp.broadcast_to(lane, (LANES, count))
    return jnp.where(hits, 1.0, 0.0).astype(jnp.bfloat16)


def publish_kernel(width, *refs):
    far, (copies, own, mass_out), near, sems, rest_refs = refs[:8], refs[8:11], refs[11:19], refs[19], refs[20:]
    moves = [pltpu.make_async_copy(a, b, sems.at[i]) for i, (a, b) in enumerate(zip(far, near))]
    for move in moves:
        move.start()
    for move in moves:
        move.wait()
    mass_out[...] = near[2][...]
    publish_body(width, *near, copies, own, *rest_refs)


def publish_body(width, old, new, mass, rest, live, live_row, bonds, send, copies, own, pub, pad, hold_a, hold_b, s_ref, row_ref):
    atoms = SUB * LANES
    sublane = lax.broadcasted_iota(jnp.int32, (SUB, LANES), 0)
    spot = lax.broadcasted_iota(jnp.int32, (SUB, LANES), 1)
    lanes = spot[0:1]

    pad[...] = jnp.zeros_like(pad)
    pad[0:6, 0:width] = send[...]
    low = pad[...]
    high = pltpu.roll(low, HALF, 1)
    ones = [low[2 * a : 2 * a + 1] + high[2 * a + 1 : 2 * a + 2] for a in range(3)]
    for a in range(3):
        pad[a : a + 1, :] = ones[a]
    index = pad[...]
    index = jnp.where(sublane < 3, index, 0)
    sent_place = (index >> 7, index & (LANES - 1))

    first_row = bonds[0:1, :]
    second_row = bonds[1:2, :]
    usable = (live_row[...] != 0) & (first_row != second_row)
    node = lax.broadcasted_iota(jnp.int32, (1, atoms), 1)
    targets = lax.broadcasted_iota(jnp.int32, (2 * SUB, atoms), 0)
    total = jnp.zeros((4 * SUB, LANES), jnp.float32)
    places = ((first_row >> 7, first_row & (LANES - 1)), second_place(second_row, width))
    marks = []
    for end, (row, lane) in enumerate(places):
        row = jnp.where(usable, row, -1)
        hits = lane_hits(lane, atoms)
        marks.append((row, hits))
        hit = targets == jnp.broadcast_to(row, targets.shape)
        total = total + nt_dot(split_codes(hit, 2 * node + end + 1), hits)
    sums = 16.0 * total[: 2 * SUB] + total[2 * SUB :]

    valid = (lanes & (HALF - 1)) < width
    slots = jnp.zeros((2 * SUB, LANES), jnp.float32)
    for a in range(3):
        row = jnp.where(valid, ones[a] >> 7, -1)
        hit = sublane == jnp.broadcast_to(row, sublane.shape)
        slots = slots + nt_dot(split_codes(hit, (SUB + a) * LANES + lanes + 1), lane_hits(ones[a] & (LANES - 1), LANES))
    sent_slot = 16.0 * slots[:SUB] + slots[SUB:]
    s_ref[0:SUB, :] = 4096.0 * sums[:SUB] + sent_slot
    out_code = sums[SUB:]

    first = stack_rows(bonds, 0, hold_a)
    second = stack_rows(bonds, 1, hold_b)
    alive = (live[...] != 0) & (first != second)
    me = sublane * LANES + spot
    none = 2 * (2 * atoms - 1)
    table = tile_rows(s_ref)
    ends = ((first >> 7, first & (LANES - 1)), second_place(second, width))
    base = 9 * SUB
    for end, (row, lane) in enumerate(ends):
        both = pick(table, row, lane).astype(jnp.int32)
        code = (both >> 12) - (2 * me + end + 1)
        ghost = both & 4095
        link = jnp.where(code > 0, code - 1, jnp.where(ghost > 0, 2 * (ghost - 1), none))
        if end == 1:
            link = jnp.where(row >= SUB, 2 * (row * LANES + lane), link)
        pub[base + end * SUB : base + (end + 1) * SUB, :] = jnp.where(alive, link, none).astype(jnp.float32)
        lead = jnp.where(alive & (2 * me + end + 1 > code), 1, 0)
        for r in range(SUB):
            row_ref[end : end + 1, r * LANES : (r + 1) * LANES] = lead[r : r + 1]
    sent = pick(table, *sent_place).astype(jnp.int32) >> 12
    in_row = (sublane < 3) & ((spot & (HALF - 1)) < width)
    darts = jnp.where(in_row, sent - 1, jnp.where(sublane >= 4, out_code.astype(jnp.int32) - 1, -1))
    tail = FIELDS * SUB
    darts = darts.astype(jnp.float32)
    pub[tail : tail + 3, :] = darts[0:3]
    pub[tail + 3 : tail + 6, :] = darts[4:7]

    total = jnp.zeros((2 * SUB, LANES), jnp.float32)
    for end, (row, hits) in enumerate(marks):
        row = jnp.where(row_ref[end : end + 1, :] != 0, row, -1)
        hit = targets[:SUB] == jnp.broadcast_to(row, (SUB, atoms))
        total = total + nt_dot(split_codes(hit, 2 * node + end + 1), hits)
    lead = 16.0 * total[:SUB] + total[SUB:]
    own[0:SUB, :] = lead.astype(jnp.int32) - 1
    own[SUB : 2 * SUB, :] = (sums[:SUB] - lead).astype(jnp.int32) - 1
    own[2 * SUB : 3 * SUB, :] = sent_slot.astype(jnp.int32) - 1

    tables = [flat_rows(old, q) for q in range(3)] + [flat_rows(new, q) for q in range(3)] + [tile_rows(mass)]
    firsts = [pick(table, *ends[0]) for table in tables]
    seconds = [pick(table, *ends[1]) for table in tables]
    heavy = pick(tables[6], *sent_place)
    for f in range(6):
        moved = pltpu.roll(heavy, (width - f * (HALF - width)) % LANES, 1)
        got = jnp.where((spot & (HALF - 1)) < width, pick(tables[f], *sent_place), moved)
        pub[tail + 6 + 3 * f : tail + 9 + 3 * f, :] = got[0:3]
    weight = live[...].astype(jnp.float32)
    away = ends[1][0] >= SUB
    span = [weight * (x - y) for x, y in zip(firsts, seconds)]
    scaling = jnp.where(away, 1.0, lax.rsqrt(firsts[6] + seconds[6]))
    norm = jnp.where(away, 1.0, lax.rsqrt(span[0] * span[0] + span[1] * span[1] + span[2] * span[2] + 0.25))
    values = [scaling * norm * span[q] for q in range(3)]
    values = values + [scaling * span[3 + q] for q in range(3)]
    values = values + [scaling * weight * rest[...], firsts[6], seconds[6]]
    for f, value in enumerate(values):
        pub[f * SUB : (f + 1) * SUB, :] = value
    block = pub[...]

    def copy(i, carry):
        copies[i] = block
        return carry

    lax.fori_loop(0, copies.shape[0], copy, 0)


def place(dart):
    return dart >> 8, (dart >> 1) & (LANES - 1)


def main_kernel(sizes, width, ranked, counts, near_list, mass, own, *refs):
    nx, ny, nz = sizes
    pubs = refs[:nx]
    (
        out_disp, out_mult, u_ref, n_ref, rho_ref, mf_ref, mg_ref, p_ref, e_ref,
        eu_ref, g_ref, w_ref, diag_ref, xa, xb, one_ref, two_ref, ea, eb, near,
    ) = refs[nx:]
    here = (lax.axis_index("gy"), lax.axis_index("gz"))
    for at, value in enumerate(near_list):
        near[at] = value
    lower = lax.broadcasted_iota(jnp.int32, (SUB, LANES), 1) < HALF

    def wrap(value, n):
        value = jnp.where(value >= n, value - n, value)
        return jnp.where(value < 0, value + n, value)

    def source(relative):
        dx, dy, dz = (d % n for d, n in zip(relative, sizes))
        return pubs[dx], wrap(here[0] + dy, ny) * nz + wrap(here[1] + dz, nz)

    def ends_of(value, dart):
        row, lane = place(dart)
        return pick({r: functools.partial(lambda r: value(r), r) for r in range(SUB)}, row, lane)

    def load(d):
        pub, s = source(ranked[d])
        field = [pub[s, f * SUB : (f + 1) * SUB, :] for f in range(FIELDS)]
        row, lane = place(field[10].astype(jnp.int32))
        away = (row >= 12) & (row < 15)
        beside = []
        for a in range(3):
            for move in (-1, 1):
                to = list(ranked[d])
                to[a] += move
                beside.append(source(to))
        def sent_row(f, a):
            at = FIELDS * SUB + 6 + 3 * f + a
            (down, i), (up, j) = beside[2 * a], beside[2 * a + 1]
            return jnp.where(lower, wide(down[i, at : at + 1, :]), wide(up[j, at : at + 1, :]))

        sent = {(f, a): sent_row(f, a) for f in range(6) for a in range(3)}
        remote = [pick({12 + a: functools.partial(sent.get, (f, a)) for a in range(3)}, row, lane) for f in range(6)]
        spare = HALF - width
        inner = lane & (HALF - 1)
        piece = sum((inner >= f * spare).astype(jnp.int32) for f in range(1, -(-width // spare)))
        tables = {16 * f + 12 + a: functools.partial(sent.get, (f, a)) for f in range(-(-width // spare)) for a in range(3)}
        remote.append(pick(tables, 16 * piece + row, (lane - inner) + width + inner - piece * spare))
        span = [field[q] - remote[q] for q in range(6)]
        mf = field[7]
        mg = jnp.where(away, remote[6], field[8])
        both = mf + mg
        scaling = lax.rsqrt(both)
        norm = scaling * lax.rsqrt(span[0] * span[0] + span[1] * span[1] + span[2] * span[2] + 0.25)
        u = [jnp.where(away, norm * span[q], field[q]) for q in range(3)]
        n = [jnp.where(away, scaling * span[3 + q], field[3 + q]) for q in range(3)]
        rho = jnp.where(away, scaling * field[6], field[6])
        root = both * scaling
        size = u[0] * u[0] + u[1] * u[1] + u[2] * u[2]
        dot = u[0] * n[0] + u[1] * n[1] + u[2] * n[2]
        value = dot * root - rho
        at = FIELDS * SUB
        darts = [pub[s, at + 3 * h : at + 3 * h + 3, :].astype(jnp.int32) for h in range(2)]

        def finish():
            diag_ref[d] = 1.0 - both * size
            xa[d] = value
            one_ref[d] = value
            for q in range(3):
                u_ref[d, q] = u[q]
                n_ref[d, q] = n[q]
            rho_ref[d] = rho
            mf_ref[d] = mf
            mg_ref[d] = mg
            p_ref[d, 0] = field[9].astype(jnp.int32)
            p_ref[d, 1] = field[10].astype(jnp.int32)
            e_ref[d] = jnp.full((SUB, LANES), -1, jnp.int32)
            e_ref[d, 0:3] = darts[0]
            e_ref[d, 4:7] = darts[1]

        return finish

    def load_ends(d):
        dart = e_ref[d]
        sign = jnp.where((dart & 1) == 1, -1.0, 1.0)
        unit = [sign * ends_of(lambda r, q=q: u_ref[d, q, r : r + 1, :], dart) for q in range(3)]
        ends = ends_of(lambda r: xa[d, r : r + 1, :], dart)

        def finish():
            ea[d] = ends
            for q in range(3):
                eu_ref[d, q] = unit[q]

        return finish

    for c in range(0, len(ranked), LOAD):
        group = range(c, min(c + LOAD, len(ranked)))
        for finish in [load(d) for d in group]:
            finish()
        for finish in [load_ends(d) for d in group]:
            finish()

    def chunks(count, body, x, ep):
        steps = -(-count // CHUNK)
        size = -(-count // steps)

        def ends(i):
            got = ends_of(lambda r: x[i, r : r + 1, :], e_ref[i])

            def finish():
                ep[i] = got

            return finish

        def step(c, carry):
            for part in (body, ends):
                for finish in [part(c * size + k) for k in range(size)]:
                    finish()
            return carry

        if steps == 1:
            step(0, 0)
        else:
            lax.fori_loop(0, steps, step, 0)

    def table_of(i, own, ghost):
        rows = {r: functools.partial(own, i, r) for r in range(SUB)}
        for a in range(3):
            table = near_list if isinstance(i, int) else near
            down, up = table[6 * i + 2 * a], table[6 * i + 2 * a + 1]

            def into(a=a, down=down, up=up):
                return jnp.where(lower, wide(ghost(up, 4 + a)), wide(ghost(down, 4 + a)))

            def away(a=a, down=down, up=up):
                return jnp.where(lower, wide(ghost(down, a)), wide(ghost(up, a)))

            rows[SUB + a] = into
            rows[SUB + 4 + a] = away
        return rows

    def pick_ends(i, tables):
        loaded = [{number: wide(make()) for number, make in table.items()} for table in tables]
        results = []
        for end in range(2):
            row, lane = place(p_ref[i, end])
            seen = [number for number in loaded[0] if end == 1 or number < SUB + 4]
            hits = {number: row == number for number in seen}
            got = []
            for data in loaded:
                total = jnp.zeros((SUB, LANES), jnp.float32)
                for number in seen:
                    value = jnp.take_along_axis(data[number], lane, axis=1, mode="promise_in_bounds")
                    total = jnp.where(hits[number], value, total)
                got.append(total)
            results.append(got)
        return results

    def pick_two(i, own, ghost):
        one, two = pick_ends(i, [table_of(i, own, ghost)])
        return one[0], two[0]

    def couple(i):
        u = [u_ref[i, q] for q in range(3)]
        mf, mg = mf_ref[i], mg_ref[i]
        signs = [mf * jnp.where((p_ref[i, 0] & 1) == 1, -1.0, 1.0), -mg * jnp.where((p_ref[i, 1] & 1) == 1, -1.0, 1.0)]
        tables = [
            table_of(i, lambda i, r, q=q: u_ref[i, q, r : r + 1, :], lambda i, r, q=q: eu_ref[i, q, r : r + 1, :])
            for q in range(3)
        ]
        tables.append(table_of(i, lambda i, r: xa[i, r : r + 1, :], lambda i, r: ea[i, r : r + 1, :]))
        value = diag_ref[i] * xa[i]
        pulls, weights = [], []
        for end, got in enumerate(pick_ends(i, tables)):
            pull = [signs[end] * got[q] for q in range(3)]
            weight = u[0] * pull[0] + u[1] * pull[1] + u[2] * pull[2]
            value = value - weight * got[3]
            pulls = pulls + pull
            weights.append(weight)
        added = one_ref[i] + value

        def finish():
            for at, pull in enumerate(pulls):
                g_ref[i, at] = pull
            for end in range(2):
                w_ref[i, end] = weights[end]
            xb[i] = value
            one_ref[i] = added

        return finish

    chunks(counts[REACH - 1], couple, xb, eb)

    def ghost_of(ep):
        return lambda i, r: ep[i, r : r + 1, :]

    def own_of(x):
        return lambda i, r: x[i, r : r + 1, :]

    def expand(state, total, reach, first, closing):
        for term in range(first, ORDER):
            (current, ep), (following, ep_next) = state
            last = term == ORDER - 1

            def body(i, current=current, ep=ep, following=following, ep_next=ep_next, last=last):
                got = pick_two(i, own_of(current), ghost_of(ep))
                value = diag_ref[i] * current[i] - w_ref[i, 0] * got[0] - w_ref[i, 1] * got[1]
                added = total[i] + value
                if last:
                    value = closing(i, added)

                def finish():
                    total[i] = added
                    following[i] = value

                return finish

            chunks(counts[reach - term - 1], body, following, ep_next)
            state = state[::-1]
        return state

    state = expand(((xb, eb), (xa, ea)), one_ref, REACH, 1, lambda i, added: added)

    def correct(i):
        (current, ep), _ = state
        got = pick_two(i, own_of(current), ghost_of(ep))
        both = mf_ref[i] + mg_ref[i]
        scaling = lax.rsqrt(both)
        mine = both * current[i]
        length = jnp.zeros((SUB, LANES), jnp.float32)
        for q in range(3):
            part = n_ref[i, q] - scaling * (u_ref[i, q] * mine + g_ref[i, q] * got[0] + g_ref[i, 3 + q] * got[1])
            length = length + part * part
        rho = rho_ref[i]
        square = rho * rho
        value = rho - jnp.sqrt(jnp.maximum(2.0 * square - length, 0.25 * square))

        def finish():
            state[1][0][i] = value
            two_ref[i] = value

        return finish

    chunks(counts[ORDER + 1], correct, *state[1])
    state = expand(state[::-1], two_ref, ORDER + 1, 0, lambda i, added: one_ref[i] + added)
    (joint, ep_ref), (spare, _) = state

    multiplier = joint[0]
    out_mult[...] = multiplier
    for q in range(3):
        spare[q] = u_ref[0, q] * multiplier
    narrow = lower[0:1]
    total = [jnp.zeros((SUB, LANES), jnp.float32)] * 3
    for end in range(2):
        dart = own[end * SUB : (end + 1) * SUB, :]
        row, lane = place(dart)
        sign = jnp.where((dart & 1) == 1, -1.0, 1.0)
        for q in range(3):
            rows = {r: functools.partial(lambda q, r: spare[q, r : r + 1, :], q, r) for r in range(SUB)}
            total[q] = total[q] + sign * pick(rows, row, lane)
    ghost = own[2 * SUB : 3 * SUB, :]
    for q in range(3):
        rows = {}
        for a in range(3):

            def make(a=a, q=q):
                down, up = near_list[2 * a], near_list[2 * a + 1]
                at = 4 + a
                from_up = eu_ref[up, q, at : at + 1, :] * ep_ref[up, at : at + 1, :]
                from_down = eu_ref[down, q, at : at + 1, :] * ep_ref[down, at : at + 1, :]
                return jnp.where(narrow, from_up, from_down)

            rows[SUB + a] = make
        value = -mass[...] * (total[q] + pick(rows, ghost >> 7, ghost & (LANES - 1)))
        for r in range(SUB):
            out_disp[q : q + 1, r * LANES : (r + 1) * LANES] = value[r : r + 1]


def domains_near(sizes):
    def far(d, n):
        return min(d, n - d)

    ranked = sorted(
        itertools.product(*(range(n) for n in sizes)), key=lambda r: (sum(far(d, n) for d, n in zip(r, sizes)), r)
    )
    span = [sum(far(d, n) for d, n in zip(r, sizes)) for r in ranked]
    ranked = [r for r, s in zip(ranked, span) if s <= REACH]
    counts = [sum(s <= d for s in span) for d in range(REACH + 1)]
    at = {r: i for i, r in enumerate(ranked)}
    near = []
    for r in ranked:
        for a in range(3):
            for move in (-1, 1):
                to = list(r)
                to[a] = (to[a] + move) % sizes[a]
                near.append(at.get(tuple(to), 0))
    return ranked, counts, near


def per_device(old_pos, new_pos, inv_mass, rest_length, bond_pairs, live, send_index):
    sizes = [lax.axis_size(axis) for axis in AXES]
    nx, ny, nz = sizes
    atoms = old_pos.shape[1]
    width = send_index.shape[1]
    tile = (SUB, LANES)
    mass, rest, alive = (v.reshape(tile) for v in (inv_mass, rest_length, live))
    f32, i32 = jnp.float32, jnp.int32
    shape = jax.ShapeDtypeStruct

    inputs = (old_pos, new_pos, mass, rest, alive, live.reshape(1, atoms), bond_pairs, send_index)
    block = (FIELDS * SUB + 24, LANES)
    pub, own, mass = pl.pallas_call(
        functools.partial(publish_kernel, width),
        out_shape=[shape((ny * nz,) + block, f32), shape((3 * SUB, LANES), i32), shape(tile, f32)],
        in_specs=[pl.BlockSpec(memory_space=pltpu.MemorySpace.HBM)] * len(inputs),
        out_specs=[VMEM] * 3,
        scratch_shapes=[pltpu.VMEM(v.shape, v.dtype) for v in inputs]
        + [pltpu.SemaphoreType.DMA((len(inputs),)), pltpu.VMEM(block, f32)]
        + [pltpu.VMEM(tile, i32)] * 3
        + [pltpu.VMEM(tile, f32), pltpu.VMEM((2, atoms), i32)],
        name="publish",
    )(*inputs)

    gathered = lax.all_to_all(pub, ("gy", "gz"), 0, 0)
    parts = [gathered]
    for d in range(1, nx):
        parts.append(lax.ppermute(gathered, "gx", [(i, (i - d) % nx) for i in range(nx)]))

    ranked, counts, near = domains_near(sizes)
    held = len(ranked) + CHUNK
    near = near + [0] * (6 * (held - len(ranked)))

    def keep(*lead, kind=f32):
        return pltpu.VMEM(lead + tile, kind)

    disp, mult = pl.pallas_call(
        functools.partial(main_kernel, sizes, width, ranked, counts, near),
        out_shape=[shape((3, atoms), f32), shape(tile, f32)],
        in_specs=[VMEM] * (2 + nx),
        out_specs=[VMEM] * 2,
        scratch_shapes=[
            keep(held, 3), keep(held, 3), keep(held), keep(held), keep(held), keep(held, 2, kind=i32), keep(held, kind=i32),
            keep(held, 3), keep(held, 6), keep(held, 2), keep(held), keep(held), keep(held), keep(held), keep(held), keep(held), keep(held),
            pltpu.SMEM((len(near),), i32),
        ],
        compiler_params=pltpu.CompilerParams(vmem_limit_bytes=24 << 20),
        name="solve",
    )(mass, own, *parts)
    return disp, mult.reshape(atoms)


def solution(mesh):
    flat = P(AXES)
    rows = P(None, AXES)
    return jax.shard_map(
        per_device,
        mesh=mesh,
        in_specs=(rows, rows, flat, flat, rows, flat, P(AXES, None)),
        out_specs=(rows, flat),
        check_vma=False,
    )
```
